32 devices in a mesh: samp: 8 (over y, x, core), par: 4 (over z).
Axes of the slice: x: 2, y: 2, z: 4, core: 2. Of those that a mesh axis runs over, the one named last changes fastest.
Arguments:
- log_derivs: bfloat16 [512, 262144], P('samp', 'par')
- energies: float32 [512, 8], P('samp'), may hold values from -6 to 6
- nys_rows: int32 [8, 8], P('samp'), may hold values from 0 to 63, as said below
Outputs:
- update: float32 [262144, 8], P('par')
- solution: float32 [512, 8], P('samp')
The draws below stay inside these ranges and needn't reach their ends.
Inputs may be any that keep to these rules, and one draw needn't show every extreme that they name: `nys_rows`: each row holds 8 different local sample numbers of that group.
All inputs are finite; a program needn't handle non-finite values.
Results may differ from the reference program's by a relative error of at most 0.014.
Values may be sent and summed in bfloat16 or wider, within the bound.
A program may use at most 128 MiB of HBM per device.

```python
import math
import jax
import jax.numpy as jnp
from jax import lax

SAMP_DEV = 64
PAR_DEV = 65536
NV = 8
RANK_DEV = 8
ITERS = 2
GROUPS = 8
NS = 512
NP = 262144
RANK = 64
N_PAR = 4


def draw_log_derivs(key, part):
    subkeys = jax.random.split(jax.random.fold_in(key, 11), 6)
    row_scale = jnp.exp(jax.random.uniform(subkeys[0], (NS, 1), jnp.float32, 0.0, math.log(10.0)))
    col_scale = jnp.exp(jax.random.uniform(subkeys[1], (1, NP), jnp.float32, math.log(0.5), math.log(2.0)))
    offset = 2.0 * jax.random.normal(subkeys[2], (1, NP), jnp.float32)
    latent_count = max(NS // 8, 8)
    latent = jax.random.normal(subkeys[4], (NS, latent_count), jnp.float32)
    loading = jax.random.normal(subkeys[5], (latent_count, NP), jnp.float32) * (0.5 / math.sqrt(latent_count))
    shared = jnp.dot(latent, loading)
    fluctuation = jax.random.normal(subkeys[3], (NS, NP), jnp.float32)
    return (offset + row_scale * (col_scale * fluctuation + shared)).astype(jnp.bfloat16)


def draw_nys_rows(key, part):
    subkeys = jax.random.split(jax.random.fold_in(key, 7), GROUPS)

    def pick_rows(subkey):
        return jax.random.permutation(subkey, SAMP_DEV)[:RANK_DEV]
    return jax.vmap(pick_rows)(subkeys).astype(jnp.int32)


def block_levels(own_key, extent, cuts, low, top_value):
    factor_of, own = 1.0, jax.random.fold_in(own_key, 6)
    for position, shards_of in cuts:
        heights = jnp.exp(jax.random.uniform(jax.random.fold_in(own, position), (shards_of,), jnp.float32, low / len(cuts), top_value / len(cuts)))
        factor_of = factor_of * jnp.repeat(heights, extent[position] // shards_of).reshape([-1 if axis == position else 1 for axis in range(len(extent))])
    return factor_of


def scatter_about(stream_key, extent, spread, bound, cuts=(), kind=jnp.bfloat16):
    gain = block_levels(stream_key, extent, cuts, -0.22, 0.18) if cuts else 1.0
    drawn = jax.random.normal(stream_key, extent, jnp.float32) * spread * gain
    return jnp.minimum(jnp.maximum(drawn, -bound), bound).astype(kind)


def setup_inputs(seed: int = 0) -> dict:
    splits = jax.random.split(jax.random.key(seed), 4)
    log_derivs = draw_log_derivs(jax.random.fold_in(splits[3], 71), 0)
    energies = scatter_about(splits[1], (NS, NV), 1.0, 6.0, ((0, 8),), jnp.float32)
    nys_rows = draw_nys_rows(jax.random.fold_in(splits[3], 71), 0)
    return {"log_derivs": log_derivs, "energies": energies, "nys_rows": nys_rows}


damping = 0.5

def centered_block(log_derivs, index):
    block = lax.dynamic_slice_in_dim(log_derivs, (index * PAR_DEV).astype(jnp.int32), PAR_DEV, 1).astype(jnp.float32)
    column_mean = lax.optimization_barrier(jnp.sum(block, axis=0)) / NS
    return ((block - column_mean) * (1.0 / math.sqrt(NP))).astype(jnp.bfloat16)

def factor_solve(factor, right):
    middle = lax.linalg.triangular_solve(factor, right, left_side=True, lower=True)
    return lax.linalg.triangular_solve(factor, middle, left_side=True, lower=True, transpose_a=True)

def small_solve(matrix, right):
    return factor_solve(jnp.linalg.cholesky(matrix), right)

def hdot(left, right):
    return jnp.dot(left, right, precision=lax.Precision.HIGHEST)

def reference(log_derivs, energies, nys_rows):
    selected = (jnp.arange(GROUPS, dtype=jnp.int32)[:, None] * SAMP_DEV + nys_rows).reshape(-1).astype(jnp.int32)
    indices = jnp.arange(N_PAR, dtype=jnp.int32)

    def add_sketch(total, index):
        block = centered_block(log_derivs, index)
        chosen = jnp.take(block, selected, axis=0)
        return (total + jnp.dot(block.astype(jnp.float32), chosen.T.astype(jnp.float32), preferred_element_type=jnp.float32), None)
    sketch, unused = lax.scan(add_sketch, jnp.zeros((NS, RANK), jnp.float32), indices)
    core_block = jnp.take(sketch, selected, axis=0)
    inner_matrix = damping * core_block + hdot(sketch.T, sketch)
    factor = jnp.linalg.cholesky(inner_matrix)

    def precondition(residual):
        coeffs = factor_solve(factor, hdot(sketch.T, residual))
        result = (residual - hdot(sketch, coeffs)) / damping
        return (result, hdot(result.T, residual))

    def apply_kernel(direction):
        rounded = direction.astype(jnp.bfloat16)

        def add_image(total, index):
            block = centered_block(log_derivs, index)
            projected = jnp.dot(block.T.astype(jnp.float32), rounded.astype(jnp.float32), preferred_element_type=jnp.float32)
            return (total + hdot(block.astype(jnp.float32), projected), None)
        images, unused_two = lax.scan(add_image, jnp.zeros((NS, NV), jnp.float32), indices)
        return images + damping * direction
    solution = jnp.zeros((NS, NV), jnp.float32)
    residual = energies
    precond_res, inner_prev = precondition(residual)
    direction = precond_res
    for iteration in range(ITERS):
        image_k = apply_kernel(direction)
        curvature = hdot(direction.T, image_k)
        alpha_k = small_solve(curvature, inner_prev)
        solution = solution + hdot(direction, alpha_k)
        if iteration + 1 < ITERS:
            residual = residual - hdot(image_k, alpha_k)
            precond_res, inner_next = precondition(residual)
            beta_k = small_solve(inner_prev, inner_next)
            direction = precond_res + hdot(direction, beta_k)
            inner_prev = inner_next
    rounded_sol = solution.astype(jnp.bfloat16)

    def update_block(index):
        block = centered_block(log_derivs, index)
        return jnp.dot(block.T.astype(jnp.float32), rounded_sol.astype(jnp.float32), preferred_element_type=jnp.float32)
    update = lax.map(update_block, indices).reshape(NP, NV)
    return (update, solution)
```

```python
import functools
import math

import jax
import jax.numpy as jnp
from jax import lax
from jax.experimental import pallas as pl
from jax.experimental.pallas import tpu as pltpu
from jax.sharding import PartitionSpec as P

ITERS = 2


damping = 0.5

MESH = pl.DeviceIdType.MESH


def factor_solve(factor, right):
    middle = lax.linalg.triangular_solve(factor, right, left_side=True, lower=True)
    return lax.linalg.triangular_solve(factor, middle, left_side=True, lower=True, transpose_a=True)


def eliminate_kernel(matrix_ref, right_ref, out_ref):
    left, right = matrix_ref[...], right_ref[...]
    row = lax.broadcasted_iota(jnp.int32, left.shape, 0)
    for i in range(left.shape[0]):
        column = left[:, i:i + 1]
        pivot = left[i:i + 1, i:i + 1]
        left_row = left[i:i + 1, :] / pivot
        right_row = right[i:i + 1, :] / pivot
        left = jnp.where(row == i, left_row, left - column * left_row)
        right = jnp.where(row == i, right_row, right - column * right_row)
    out_ref[...] = right


def small_solve(matrix, right):
    matrix = 0.5 * (matrix + matrix.T)
    return pl.pallas_call(
        eliminate_kernel, out_shape=jax.ShapeDtypeStruct(right.shape, right.dtype)
    )(matrix, right)


def hdot(left, right):
    return jnp.dot(left, right, precision=lax.Precision.HIGHEST)


def greet(peers):
    barrier = pltpu.get_barrier_semaphore()
    for peer in peers:
        pl.semaphore_signal(barrier, inc=1, device_id=peer, device_id_type=MESH)
    pl.semaphore_wait(barrier, len(peers))


def remote(src, dst, send, recv, peer):
    return pltpu.make_async_remote_copy(
        src_ref=src, dst_ref=dst, send_sem=send, recv_sem=recv, device_id=peer, device_id_type=MESH
    )


def gather_kernel(n, total_rows, scale, sums_ref, aux_ref, chosen_ref, full_ref, sketch_ref, aux_out, centered_out,
                  mean_ref, rows_out, centered_ref, land, own, full, s1, r1, s2, r2, s3, r3, s4, r4, s5, r5, s6, r6, local):
    me, col = lax.axis_index("samp"), lax.axis_index("par")
    at = [lax.rem(me + k, n) for k in range(n)]
    back = [lax.rem(me + n - k, n) for k in range(n)]
    peer = [(at[k], col) for k in range(n)]
    pair = (jnp.bitwise_xor(me, 1), col)
    width = chosen_ref.shape[1]
    half = width // 2
    part = [pl.ds(0, half), pl.ds(half, half)]
    load = pltpu.make_async_copy(full_ref, full, local.at[2])
    load.start()
    greet(peer[1:])
    scatter = [remote(sums_ref.at[at[k]], land.at[k], s1.at[k], r1.at[k], peer[k]) for k in range(1, n)]
    for copy in scatter:
        copy.start()
    sent = list(scatter)
    quad = n == 8
    beside = [jnp.bitwise_xor(me, 2), jnp.bitwise_xor(me, 4)]
    if quad:
        first = [
            remote(chosen_ref.at[:, part[d]], rows_out.at[me, :, part[d]], s4.at[d], r4.at[d], (beside[d], col))
            for d in range(2)
        ]
        for copy in first:
            copy.start()
        sent += first
    auxes = [remote(aux_ref, aux_out.at[me], s2.at[k], r2.at[k], peer[k]) for k in range(1, n)]
    mine = pltpu.make_async_copy(aux_ref, aux_out.at[me], local.at[0])
    mine.start()
    keep = pltpu.make_async_copy(chosen_ref, rows_out.at[me], local.at[1])
    keep.start()
    total = sums_ref[me]
    for k in range(1, n):
        scatter[k - 1].wait_recv()
        total = total + land[k]
    own[...] = total / total_rows
    mean_ref[me] = own[...]
    spread = [remote(own, mean_ref.at[me], s3.at[k], r3.at[k], peer[k]) for k in range(1, n)]
    for copy in spread + auxes:
        copy.start()
    sent += spread + auxes
    over = [remote(chosen_ref, rows_out.at[me], s5.at[0], r5.at[0], pair)]
    over[0].start()
    if quad:
        second = [
            remote(chosen_ref.at[:, part[1 - d]], rows_out.at[me, :, part[1 - d]], s4.at[2 + d], r4.at[2 + d],
                   (beside[d], col))
            for d in range(2)
        ]
        for copy in second:
            copy.start()
        sent += second
        for d in range(2):
            view = rows_out.at[beside[d], :, part[d]]
            remote(view, view, s4.at[d], r4.at[d], pair).wait_recv()
            step = remote(view, view, s4.at[4 + d], r4.at[4 + d], (beside[1 - d], col))
            step.start()
            sent.append(step)
    else:
        far = [remote(chosen_ref, rows_out.at[me], s4.at[k], r4.at[k], peer[k]) for k in range(2, n, 2)]
        for copy in far:
            copy.start()
        sent += far
    for k in range(1, n):
        remote(own, mean_ref.at[back[k]], s3.at[k], r3.at[k], peer[k]).wait_recv()
    load.wait()
    slab = width // n
    tile = math.gcd(slab, 1024)

    @pl.loop(0, n)
    def _(j):
        @pl.loop(0, slab // tile)
        def _(t):
            inner = pl.multiple_of(t * tile, tile)
            cols = pl.ds(pl.multiple_of(j * slab + inner, tile), tile)
            mean = mean_ref[j, :, pl.ds(inner, tile)]
            centered_ref[:, cols] = ((full[:, cols].astype(jnp.float32) - mean) * scale).astype(jnp.bfloat16)

    put = pltpu.make_async_copy(centered_ref, centered_out, local.at[2])
    put.start()
    if quad:
        for d in range(2):
            view = rows_out.at[beside[d], :, part[1 - d]]
            remote(view, view, s4.at[2 + d], r4.at[2 + d], pair).wait_recv()
            block = rows_out.at[beside[d]]
            step = remote(block, block, s5.at[1 + d], r5.at[1 + d], pair)
            step.start()
            over.append(step)
        cross = jnp.bitwise_xor(me, 6)
        for d in range(2):
            view = rows_out.at[cross, :, part[d]]
            remote(view, view, s4.at[4 + d], r4.at[4 + d], pair).wait_recv()
            step = remote(view, view, s5.at[3 + d], r5.at[3 + d], pair)
            step.start()
            over.append(step)
        block = rows_out.at[jnp.bitwise_xor(me, 1)]
        remote(block, block, s5.at[0], r5.at[0], pair).wait_recv()
        for d in range(2):
            block = rows_out.at[jnp.bitwise_xor(me, 3 + 2 * d)]
            remote(block, block, s5.at[1 + d], r5.at[1 + d], pair).wait_recv()
            view = rows_out.at[jnp.bitwise_xor(me, 7), :, part[d]]
            remote(view, view, s5.at[3 + d], r5.at[3 + d], pair).wait_recv()
    else:
        for k in range(2, n, 2):
            block = rows_out.at[back[k]]
            remote(block, block, s4.at[k], r4.at[k], pair).wait_recv()
            step = remote(block, block, s5.at[k], r5.at[k], pair)
            step.start()
            over.append(step)
        for k in range(0, n, 2):
            block = rows_out.at[lax.rem(pair[0] + n - k, n)]
            remote(block, block, s5.at[k], r5.at[k], pair).wait_recv()
    for k in range(1, n):
        remote(aux_ref, aux_out.at[back[k]], s2.at[k], r2.at[k], peer[k]).wait_recv()
    for copy in sent + over:
        copy.wait_send()
    mine.wait()
    keep.wait()
    sketch_ref[...] = jnp.zeros_like(sketch_ref)
    count = n * chosen_ref.shape[0]

    @pl.loop(0, n)
    def _(j):
        @pl.loop(0, slab // tile)
        def _(t):
            inner = pl.multiple_of(t * tile, tile)
            cols = pl.ds(pl.multiple_of(j * slab + inner, tile), tile)
            mean = mean_ref[j, :, pl.ds(inner, tile)]
            rows = rows_out[:, :, cols].astype(jnp.float32).reshape(count, tile)
            rows = ((rows - mean) * scale).astype(jnp.bfloat16)
            sketch_ref[...] += lax.dot_general(
                centered_ref[:, cols], rows, (((1,), (1,)), ((), ())), preferred_element_type=jnp.float32
            )

    put.wait()


def gather_rows(sums, aux, chosen, full, n, total_rows, scale, ident):
    dma = lambda: pltpu.SemaphoreType.DMA((n,))
    vmem = pl.BlockSpec(memory_space=pltpu.VMEM)
    slab = sums.shape[-1]
    return pl.pallas_call(
        functools.partial(gather_kernel, n, total_rows, scale),
        out_shape=(
            jax.ShapeDtypeStruct((full.shape[0], n * chosen.shape[0]), jnp.float32),
            jax.ShapeDtypeStruct((n,) + aux.shape, jnp.float32),
            jax.ShapeDtypeStruct(full.shape, full.dtype),
        ),
        in_specs=[vmem, vmem, vmem, pl.BlockSpec(memory_space=pl.ANY)],
        out_specs=(vmem, vmem, pl.BlockSpec(memory_space=pl.ANY)),
        scratch_shapes=[
            pltpu.VMEM(sums.shape, jnp.float32),
            pltpu.VMEM((n,) + chosen.shape, chosen.dtype),
            pltpu.VMEM(full.shape, full.dtype),
            pltpu.VMEM(sums.shape, jnp.float32),
            pltpu.VMEM((1, slab), jnp.float32),
            pltpu.VMEM(full.shape, full.dtype),
        ] + [dma() for _ in range(12)] + [pltpu.SemaphoreType.DMA((3,))],
        compiler_params=pltpu.CompilerParams(
            collective_id=ident, has_side_effects=True, vmem_limit_bytes=60 * 2**20
        ),
    )(sums, aux, chosen, full)


def spread_kernel(n, p, part_ref, out_ref, land, own, s1, r1, s2, r2):
    me, col = lax.axis_index("samp"), lax.axis_index("par")
    beside = [lax.rem(col + k, p) for k in range(p)]
    at = [lax.rem(me + k, n) for k in range(n)]
    back = [lax.rem(me + n - k, n) for k in range(n)]
    greet([(me, beside[k]) for k in range(1, p)] + [(at[k], col) for k in range(1, n)])
    sums = [remote(part_ref, land.at[col], s1.at[k], r1.at[k], (me, beside[k])) for k in range(1, p)]
    for copy in sums:
        copy.start()
    land[col] = part_ref[...]
    for k in range(1, p):
        there = lax.rem(col + p - k, p)
        remote(part_ref, land.at[there], s1.at[k], r1.at[k], (me, beside[k])).wait_recv()
    total = land[0]
    for j in range(1, p):
        total = total + land[j]
    own[...] = total
    out_ref[me] = total
    hops = [remote(own, out_ref.at[me], s2.at[k], r2.at[k], (at[k], col)) for k in range(1, n)]
    for copy in hops:
        copy.start()
    for k in range(1, n):
        remote(own, out_ref.at[back[k]], s2.at[k], r2.at[k], (at[k], col)).wait_recv()
    for copy in sums + hops:
        copy.wait_send()


def sum_and_spread(part, n, p, ident):
    vmem = pl.BlockSpec(memory_space=pltpu.VMEM)
    return pl.pallas_call(
        functools.partial(spread_kernel, n, p),
        out_shape=jax.ShapeDtypeStruct((n,) + part.shape, jnp.float32),
        in_specs=[vmem],
        out_specs=vmem,
        scratch_shapes=[
            pltpu.VMEM((p,) + part.shape, jnp.float32),
            pltpu.VMEM(part.shape, jnp.float32),
            pltpu.SemaphoreType.DMA((p,)),
            pltpu.SemaphoreType.DMA((p,)),
            pltpu.SemaphoreType.DMA((n,)),
            pltpu.SemaphoreType.DMA((n,)),
        ],
        compiler_params=pltpu.CompilerParams(collective_id=ident, has_side_effects=True),
    )(part)


def reduce_kernel(n, part_ref, out_ref, land, both, inbox, s0, r0, s1, r1, s2, r2, s3, r3):
    me, col = lax.axis_index("samp"), lax.axis_index("par")
    outer = n // 2
    slab = part_ref.shape[1] // n
    half = slab * outer
    i, o = lax.rem(me, 2), me // 2
    pair = (jnp.bitwise_xor(me, 1), col)
    at = [lax.rem(o + k, outer) for k in range(outer)]
    back = [lax.rem(o + outer - k, outer) for k in range(outer)]
    peer = [(at[k] * 2 + i, col) for k in range(outer)]
    cols = lambda j: pl.ds(pl.multiple_of(j * slab, slab), slab)
    halves = lambda j: pl.ds(pl.multiple_of(j * half, half), half)
    greet([pair] + peer[1:])
    swap = remote(part_ref.at[:, halves(1 - i)], land, s0.at[0], r0.at[0], pair)
    swap.start()
    swap.wait_recv()
    both[...] = (part_ref[:, halves(i)].astype(jnp.float32) + land[...].astype(jnp.float32)).astype(both.dtype)
    scatter = [remote(both.at[:, cols(at[k])], inbox.at[k], s1.at[k], r1.at[k], peer[k]) for k in range(1, outer)]
    for copy in scatter:
        copy.start()
    total = part_ref[:, cols(i * outer + o)].astype(jnp.float32) + land[:, cols(o)].astype(jnp.float32)
    for k in range(1, outer):
        scatter[k - 1].wait_recv()
        total = total + inbox[k].astype(jnp.float32)
    home = cols(i * outer + o)
    out_ref[:, home] = total.astype(out_ref.dtype)
    mine = out_ref.at[:, home]
    spread = [remote(mine, mine, s2.at[k], r2.at[k], peer[k]) for k in range(1, outer)]
    spread.append(remote(mine, mine, s3.at[0], r3.at[0], pair))
    for copy in spread:
        copy.start()
    for k in range(1, outer):
        block = out_ref.at[:, cols(i * outer + back[k])]
        remote(block, block, s2.at[k], r2.at[k], pair).wait_recv()
        step = remote(block, block, s3.at[k], r3.at[k], pair)
        step.start()
        spread.append(step)
    for k in range(outer):
        block = out_ref.at[:, cols((1 - i) * outer + back[k])]
        remote(block, block, s3.at[k], r3.at[k], pair).wait_recv()
    for copy in [swap] + scatter + spread:
        copy.wait_send()


def reduce_all(part, n, ident):
    count, width = part.shape
    outer = n // 2
    vmem = pl.BlockSpec(memory_space=pltpu.VMEM)
    return pl.pallas_call(
        functools.partial(reduce_kernel, n),
        out_shape=jax.ShapeDtypeStruct(part.shape, part.dtype),
        in_specs=[vmem],
        out_specs=vmem,
        scratch_shapes=[
            pltpu.VMEM((count, width // 2), part.dtype),
            pltpu.VMEM((count, width // 2), part.dtype),
            pltpu.VMEM((outer, count, width // n), part.dtype),
        ]
        + [pltpu.SemaphoreType.DMA((outer,)) for _ in range(8)],
        compiler_params=pltpu.CompilerParams(collective_id=ident, has_side_effects=True),
    )(part)


def tiny_kernel(p, part_ref, out_ref, land, s1, r1):
    me, col = lax.axis_index("samp"), lax.axis_index("par")
    at = [lax.rem(col + k, p) for k in range(p)]
    back = [lax.rem(col + p - k, p) for k in range(p)]
    greet([(me, at[k]) for k in range(1, p)])
    copies = [remote(part_ref, land.at[col], s1.at[k], r1.at[k], (me, at[k])) for k in range(1, p)]
    for copy in copies:
        copy.start()
    land[col] = part_ref[...]
    for k in range(1, p):
        remote(part_ref, land.at[back[k]], s1.at[k], r1.at[k], (me, at[k])).wait_recv()
    for copy in copies:
        copy.wait_send()
    total = land[0]
    for j in range(1, p):
        total = total + land[j]
    out_ref[...] = total


def tiny_sum(part, p, ident):
    vmem = pl.BlockSpec(memory_space=pltpu.VMEM)
    return pl.pallas_call(
        functools.partial(tiny_kernel, p),
        out_shape=jax.ShapeDtypeStruct(part.shape, part.dtype),
        in_specs=[vmem],
        out_specs=vmem,
        scratch_shapes=[pltpu.VMEM((p,) + part.shape, part.dtype)]
        + [pltpu.SemaphoreType.DMA((p,)) for _ in range(2)],
        compiler_params=pltpu.CompilerParams(collective_id=ident, has_side_effects=True),
    )(part)


def general_body(log_derivs, energies, nys_rows):
    rows, width = log_derivs.shape
    n, p = lax.axis_size("samp"), lax.axis_size("par")
    count, rank = energies.shape[1], nys_rows.shape[1]
    scale = 1.0 / math.sqrt(width * p)
    picks = (nys_rows.reshape(rank, 1) == lax.broadcasted_iota(jnp.int32, (rank, rows), 1)).astype(jnp.bfloat16)
    probe = jnp.concatenate([picks, jnp.ones((8, rows), jnp.bfloat16)], axis=0)
    taken = jnp.dot(probe, log_derivs, preferred_element_type=jnp.float32)
    chosen = taken[:rank].astype(jnp.bfloat16)
    sums = taken[rank].reshape(n, 1, width // n)
    aux = jnp.concatenate([energies, picks.astype(jnp.float32).T], axis=1)
    sketch_part, aux_all, centered = gather_rows(sums, aux, chosen, log_derivs, n, n * rows, scale, 0)
    sketch = sum_and_spread(sketch_part, n, p, 1).reshape(n * rows, n * rank)
    all_energies = aux_all[:, :, :count].reshape(n * rows, count)
    core_block = jnp.einsum(
        "grj,grk->gjk", aux_all[:, :, count:], sketch.reshape(n, rows, n * rank), precision=lax.Precision.HIGHEST
    ).reshape(n * rank, n * rank)
    factor = jnp.linalg.cholesky(damping * core_block + hdot(sketch.T, sketch))

    def precondition(residual):
        coeffs = factor_solve(factor, hdot(sketch.T, residual))
        result = (residual - hdot(sketch, coeffs)) / damping
        return (result, hdot(result.T, residual))

    start = lax.axis_index("samp") * rows
    solution = jnp.zeros(all_energies.shape, jnp.float32)
    update = 0.0
    residual = all_energies
    precond_res, inner_prev = precondition(residual)
    direction = precond_res
    for iteration in range(ITERS):
        rounded = lax.dynamic_slice_in_dim(direction, start, rows, 0).astype(jnp.bfloat16)
        part = jnp.einsum("rv,rc->vc", rounded, centered, preferred_element_type=jnp.float32)
        projected = reduce_all(part.astype(jnp.bfloat16), n, 2 + 2 * iteration)
        if iteration + 1 < ITERS:
            image_part = jnp.einsum("rc,vc->vr", centered, projected, preferred_element_type=jnp.float32)
            image_k = sum_and_spread(image_part, n, p, 3 + 2 * iteration)
            image_k = image_k.transpose(0, 2, 1).reshape(n * rows, count) + damping * direction
            curvature = hdot(direction.T, image_k)
        else:
            square = jnp.einsum("uc,vc->uv", projected, projected, preferred_element_type=jnp.float32)
            curvature = tiny_sum(square, p, 3 + 2 * iteration) + damping * hdot(direction.T, direction)
        alpha_k = small_solve(curvature, inner_prev)
        solution = solution + hdot(direction, alpha_k)
        update = update + hdot(alpha_k.T, projected.astype(jnp.float32))
        if iteration + 1 < ITERS:
            residual = residual - hdot(image_k, alpha_k)
            precond_res, inner_next = precondition(residual)
            beta_k = small_solve(inner_prev, inner_next)
            direction = precond_res + hdot(direction, beta_k)
            inner_prev = inner_next
    return (update.T, lax.dynamic_slice_in_dim(solution, start, rows, 0))


CHUNKS = 16
EARLY = 4
AHEAD = 8
LAG = 2


def contract_last(left, right, precision=None):
    return lax.dot_general(
        left, right, (((1,), (1,)), ((), ())), precision=precision, preferred_element_type=jnp.float32
    )


def exact(left, right):
    return jnp.dot(left, right, precision=lax.Precision.HIGHEST, preferred_element_type=jnp.float32)


def exact_t(left, right):
    return contract_last(left, right, lax.Precision.HIGHEST)


def places():
    me, z = lax.axis_index("samp"), lax.axis_index("par")
    c, q = lax.rem(me, 2), me // 2
    near = [jnp.bitwise_xor(q, 1), jnp.bitwise_xor(q, 2)]
    return me, z, c, 1 - c, q, near, jnp.bitwise_xor(q, 3)


def sketch_kernel(p, total_rows, scale, x_ref, probe_ref, aux_ref, sk_ref, aux_out, c_out, stage, xh, other, rin,
                  sums, sland, acc1, acc2, mean, acc, pland, mine, zland, tot, lsem, wsem, wrecv, osem, psem, rsem,
                  fsem, drecv, bsem, brecv, asem, arecv, tsem, trecv, csem, local):
    me, z, c, o, q, near, far = places()
    rows, half = stage.shape
    width = half // CHUNKS
    count = rin.shape[1]
    dev = lambda chip, core: (chip * 2 + core, z)
    pair = dev(q, o)
    span = lambda k: pl.ds(pl.multiple_of(k * width, width), width)

    def load(k, own):
        core = c if own else o
        cols = pl.ds(pl.multiple_of(core * half + k * width, width), width)
        dst = xh.at[c, :, span(k)] if own else stage.at[:, span(k)]
        return pltpu.make_async_copy(x_ref.at[:, cols], dst, lsem.at[int(own), k])

    @pl.loop(0, CHUNKS)
    def _(k):
        load(k, False).start()
        load(k, True).start()

    samp_peers = [(lax.rem(me + k, 8), z) for k in range(1, 8)]
    par_peers = [(me, lax.rem(z + k, p)) for k in range(1, p)]
    greet(samp_peers + par_peers)
    auxes = [remote(aux_ref, aux_out.at[me], asem.at[k], arecv.at[k], samp_peers[k]) for k in range(7)]
    for copy in auxes:
        copy.start()
    keep = pltpu.make_async_copy(aux_ref, aux_out.at[me], local.at[0])
    keep.start()

    def swap(k):
        return remote(stage.at[:, span(k)], xh.at[c, :, span(k)], wsem.at[k], wrecv.at[k], pair)

    def to_pair(k):
        return remote(other.at[:, span(k)], rin.at[me, :, span(k)], psem.at[k], rsem.at[me, k], pair)

    def direct(k):
        view = rin.at[me, :, span(k)]
        found = []
        for d in range(2):
            found.append(remote(view, view, osem.at[d, k], rsem.at[me, k], dev(near[d], c)))
            found.append(remote(other.at[:, span(k)], view, osem.at[2 + d, k], rsem.at[me, k], dev(near[d], o)))
        return found

    def forward(k, d):
        view = rin.at[pl.ds(pl.multiple_of(near[d] * 2, 2), 2), :, span(k)]
        return remote(view, view, fsem.at[k], drecv.at[k], dev(near[1 - d], c))

    def send(k):
        for copy in direct(k):
            copy.start()

    def extract(k):
        for own in (False, True):
            load(k, own).wait()
            step = min(width, 1024)
            for s in range(width // step):
                cols = pl.ds(pl.multiple_of(k * width + s * step, step), step)
                block = xh[c, :, cols] if own else stage[:, cols]
                taken = jnp.dot(probe_ref[...], block, preferred_element_type=jnp.float32)
                if own:
                    rin[me, :, cols] = taken[:count].astype(rin.dtype)
                    sums[c, :, cols] = taken[count:count + 1]
                else:
                    other[:, cols] = taken[:count].astype(other.dtype)
                    sums[o, :, cols] = taken[count:count + 1]
            if not own:
                swap(k).start()
                to_pair(k).start()

    @pl.loop(0, EARLY)
    def _(k):
        extract(k)
        send(k)

    @pl.loop(EARLY, CHUNKS)
    def _(k):
        extract(k)

    first = remote(sums.at[o], sland.at[0], bsem.at[0], brecv.at[0], pair)
    first.start()
    first.wait_recv()
    acc1[...] = sums[c] + sland[0]
    part = [pl.ds(0, half // 2), pl.ds(half // 2, half // 2)]
    second = [
        remote(acc1.at[:, part[d]], sland.at[1, :, part[d]], bsem.at[1 + d], brecv.at[1 + d], dev(near[d], c))
        for d in range(2)
    ]
    for copy in second:
        copy.start()

    middle = (EARLY + AHEAD) // 2

    @pl.loop(EARLY, middle)
    def _(k):
        send(k)

    for copy in second:
        copy.wait_recv()
    acc2[...] = acc1[...] + sland[1]
    third = [
        remote(acc2.at[:, part[d]], sland.at[2, :, part[d]], bsem.at[3 + d], brecv.at[3 + d], dev(near[1 - d], c))
        for d in range(2)
    ]
    for copy in third:
        copy.start()

    @pl.loop(middle, AHEAD)
    def _(k):
        send(k)

    for copy in third:
        copy.wait_recv()
    mean[...] = (acc2[...] + sland[2]) / total_rows
    acc[...] = jnp.zeros_like(acc)

    def arrived(k):
        for d in range(2):
            for core in range(2):
                g = near[d] * 2 + core
                view = rin.at[g, :, span(k)]
                remote(view, view, fsem.at[k], rsem.at[g, k], pair).wait_recv()

    def process(k):
        remote(stage.at[:, span(k)], xh.at[o, :, span(k)], wsem.at[k], wrecv.at[k], pair).wait_recv()
        g = me + 1 - 2 * c
        view = rin.at[g, :, span(k)]
        remote(view, view, fsem.at[k], rsem.at[g, k], pair).wait_recv()
        view = rin.at[pl.ds(pl.multiple_of(far * 2, 2), 2), :, span(k)]
        remote(view, view, fsem.at[k], drecv.at[k], pair).wait_recv()
        step = min(width, 512)
        for s in range(width // step):
            cols = pl.ds(pl.multiple_of(k * width + s * step, step), step)
            shift = mean[:, cols]
            block = xh[:, :, cols].astype(jnp.float32).reshape(2 * rows, step)
            block = ((block - shift) * scale).astype(jnp.bfloat16)
            xh[:, :, cols] = block.reshape(2, rows, step)
            picked = rin[:, :, cols].astype(jnp.float32).reshape(8 * count, step)
            picked = ((picked - shift) * scale).astype(jnp.bfloat16)
            acc[...] += contract_last(picked, block)
        pltpu.make_async_copy(xh.at[:, :, span(k)], c_out.at[:, :, span(k)], csem.at[k]).start()

    @pl.loop(0, (CHUNKS + LAG) // 2)
    def _(i):
        for d in range(2):
            k = 2 * i + d

            @pl.when(k + AHEAD < CHUNKS)
            def _():
                send(k + AHEAD)

            @pl.when(k < CHUNKS)
            def _():
                arrived(k)
                forward(k, d).start()

            @pl.when(k >= LAG)
            def _():
                process(k - LAG)

    own_rows = acc.shape[0] // 2
    mine_rows = pl.ds(pl.multiple_of(c * own_rows, own_rows), own_rows)
    their_rows = pl.ds(pl.multiple_of(o * own_rows, own_rows), own_rows)
    give = remote(acc.at[their_rows], pland, tsem.at[0], trecv.at[0], pair)
    give.start()
    give.wait_recv()
    mine[...] = acc[mine_rows, :] + pland[...]
    across = [remote(mine, zland.at[z], tsem.at[k], trecv.at[k], par_peers[k - 1]) for k in range(1, p)]
    for copy in across:
        copy.start()
    zland[z] = mine[...]
    for k in range(1, p):
        view = zland.at[lax.rem(z + p - k, p)]
        remote(view, view, tsem.at[k], trecv.at[k], pair).wait_recv()
    total = zland[0]
    for j in range(1, p):
        total = total + zland[j]
    tot[...] = total
    spot = lambda chip, core: sk_ref.at[
        pl.ds(pl.multiple_of(core * own_rows, own_rows), own_rows),
        pl.ds(pl.multiple_of(chip * 2 * rows, 2 * rows), 2 * rows),
    ]
    sk_ref[mine_rows, pl.ds(pl.multiple_of(q * 2 * rows, 2 * rows), 2 * rows)] = total
    spread = [remote(tot, spot(q, c), tsem.at[p + k], trecv.at[p + k], samp_peers[k]) for k in range(7)]
    for copy in spread:
        copy.start()
    for k in range(7):
        source = lax.rem(me + 7 - k, 8)
        view = spot(source // 2, lax.rem(source, 2))
        remote(view, view, tsem.at[p + k], trecv.at[p + k], pair).wait_recv()
    for k in range(7):
        view = aux_out.at[lax.rem(me + 7 - k, 8)]
        remote(view, view, asem.at[k], arecv.at[k], pair).wait_recv()
    keep.wait()

    @pl.loop(0, CHUNKS // 2)
    def _(i):
        for d in range(2):
            k = 2 * i + d
            swap(k).wait_send()
            to_pair(k).wait_send()
            for copy in direct(k):
                copy.wait_send()
            forward(k, d).wait_send()
            pltpu.make_async_copy(xh.at[:, :, span(k)], c_out.at[:, :, span(k)], csem.at[k]).wait()

    for copy in auxes + [first] + second + third + [give] + across + spread:
        copy.wait_send()


def sketch_call(x, probe, aux, p, total_rows, scale, ident):
    rows, full = x.shape
    half = full // 2
    count = probe.shape[0] // 2
    vmem, hbm = pl.BlockSpec(memory_space=pltpu.VMEM), pl.BlockSpec(memory_space=pl.ANY)
    dma = lambda *shape: pltpu.SemaphoreType.DMA(shape)
    rank = 8 * count
    line = lambda k: pltpu.VMEM((k, 1, half), jnp.float32)
    return pl.pallas_call(
        functools.partial(sketch_kernel, p, total_rows, scale),
        out_shape=(
            jax.ShapeDtypeStruct((rank, 8 * rows), jnp.float32),
            jax.ShapeDtypeStruct((8,) + aux.shape, jnp.float32),
            jax.ShapeDtypeStruct((2, rows, half), x.dtype),
        ),
        in_specs=[hbm, vmem, vmem],
        out_specs=(vmem, vmem, hbm),
        scratch_shapes=[
            pltpu.VMEM((rows, half), x.dtype),
            pltpu.VMEM((2, rows, half), x.dtype),
            pltpu.VMEM((count, half), x.dtype),
            pltpu.VMEM((8, count, half), x.dtype),
            line(2),
            line(3),
            pltpu.VMEM((1, half), jnp.float32),
            pltpu.VMEM((1, half), jnp.float32),
            pltpu.VMEM((1, half), jnp.float32),
            pltpu.VMEM((rank, 2 * rows), jnp.float32),
            pltpu.VMEM((rank // 2, 2 * rows), jnp.float32),
            pltpu.VMEM((rank // 2, 2 * rows), jnp.float32),
            pltpu.VMEM((p, rank // 2, 2 * rows), jnp.float32),
            pltpu.VMEM((rank // 2, 2 * rows), jnp.float32),
            dma(2, CHUNKS), dma(CHUNKS), dma(CHUNKS), dma(4, CHUNKS), dma(CHUNKS), dma(8, CHUNKS),
            dma(CHUNKS), dma(CHUNKS), dma(5), dma(5), dma(7), dma(7), dma(p + 7), dma(p + 7), dma(CHUNKS), dma(1),
        ],
        compiler_params=pltpu.CompilerParams(
            collective_id=ident, has_side_effects=True, vmem_limit_bytes=60 * 2**20
        ),
    )(x, probe, aux)


def eliminate(matrix, size, group):
    row = lax.broadcasted_iota(jnp.int32, matrix.shape, 0)
    lanes = matrix.shape[1]
    for start in range(0, size, group):
        spread = lambda i, j: jnp.broadcast_to(matrix[start + i:start + i + 1, start + j:start + j + 1], (1, lanes))
        cell = [[spread(i, j) for j in range(group)] for i in range(group)]
        for k in range(group):
            inverse = 1.0 / cell[k][k]
            scaled = [cell[k][j] * inverse for j in range(group)]
            for i in range(group):
                if i != k:
                    factor = cell[i][k]
                    cell[i] = [cell[i][j] - factor * scaled[j] for j in range(group)]
                    cell[i][k] = -factor * inverse
            scaled[k] = inverse
            cell[k] = scaled
        old = [matrix[start + j:start + j + 1, :] for j in range(group)]
        fresh = []
        for i in range(group):
            line = cell[i][0] * old[0]
            for j in range(1, group):
                line = line + cell[i][j] * old[j]
            fresh.append(line)
        change = matrix[:, start:start + 1] * fresh[0]
        for i in range(1, group):
            change = change + matrix[:, start + i:start + i + 1] * fresh[i]
        matrix = matrix - change
        for i in range(group):
            matrix = jnp.where(row == start + i, fresh[i], matrix)
    return matrix


def solve_kernel(p, c_ref, sk_ref, aux_ref, update_ref, sol_ref, cbuf, aug, big, small, dref, rres, part, land1, mid,
                 keep, land2, pf, msg, mland, img, lsem, s1, r1, s2, r2, s3, r3, s4, r4, s5, r5, s6, r6, s7, r7):
    me, z, c, o, q, near, far = places()
    rows, half = cbuf.shape[1], cbuf.shape[2]
    quarter = half // 4
    piece = quarter // 2
    dev = lambda chip: (chip * 2 + c, z)
    pair = (q * 2 + o, z)
    pieces = CHUNKS // 2
    width = half // pieces

    def load(k):
        cols = pl.ds(k * width, width)
        return pltpu.make_async_copy(c_ref.at[:, :, cols], cbuf.at[:, :, cols], lsem.at[k])

    for k in range(pieces):
        load(k).start()
    group = [(q * 2 + lax.rem(c + k // p, 2), lax.rem(z + lax.rem(k, p), p)) for k in range(1, 2 * p)]
    chips = [dev(near[0]), dev(near[1]), dev(far)]
    greet(chips + group)

    rank = sk_ref.shape[0]
    vecs = aug.shape[0] - rank
    sketch = sk_ref[...]
    aug[pl.ds(0, rank), :] = sketch
    for g in range(8):
        cols = pl.ds((g // 2) * 2 * rows, 2 * rows)
        here = pl.ds(g * vecs, vecs)
        aug[here, cols] = aug[here, cols] + damping * aux_ref[g, vecs:, :]
    for chip in range(4):
        cols = pl.ds(chip * 2 * rows, 2 * rows)
        aug[pl.ds(rank, vecs), cols] = aux_ref[2 * chip, :vecs, :] + aux_ref[2 * chip + 1, :vecs, :]
    product = exact_t(aug[...], sketch)
    big[...] = (
        lax.broadcasted_iota(jnp.int32, big.shape, 0) + rank == lax.broadcasted_iota(jnp.int32, big.shape, 1)
    ).astype(jnp.float32)
    big[:, pl.ds(0, rank)] = product[:rank]
    inverse = eliminate(big[...], rank, 4)[:, rank:2 * rank]
    energies = aug[pl.ds(rank, vecs), :]
    dref[...] = (energies - exact(exact(product[rank:], inverse), sketch)) / damping
    gamma = exact_t(dref[...], energies)

    def small_inverse(matrix):
        small[...] = (
            lax.broadcasted_iota(jnp.int32, small.shape, 0) + vecs == lax.broadcasted_iota(jnp.int32, small.shape, 1)
        ).astype(jnp.float32)
        small[:, pl.ds(0, vecs)] = matrix
        return eliminate(small[...], vecs, 4)[:, vecs:2 * vecs]

    spot = lambda chip, s: pl.ds(pl.multiple_of(chip * quarter + s * piece, piece), piece)
    step = min(piece, 1024)

    def all_reduce(turn):
        rounded = dref[:, pl.ds(pl.multiple_of(q * 2 * rows, 2 * rows), 2 * rows)].astype(jnp.bfloat16)

        def project(chip, s):
            @pl.loop(0, piece // step)
            def _(t):
                cols = pl.ds(pl.multiple_of(chip * quarter + s * piece + t * step, step), step)
                block = cbuf[:, :, cols].reshape(2 * rows, step)
                part[turn, :, cols] = jnp.dot(rounded, block, preferred_element_type=jnp.float32).astype(part.dtype)

        sends = []
        for j, target in enumerate((lambda d: far, lambda d: near[d])):
            for d in range(2):
                chip = target(d)
                project(chip, d)
                copy = remote(part.at[turn, :, spot(chip, d)], land1.at[turn, d, j], s1.at[turn, d, j],
                              r1.at[turn, d, j], dev(near[d]))
                copy.start()
                sends.append(copy)
        for d in range(2):
            project(near[1 - d], d)
        for d in range(2):
            project(q, d)
        for d in range(2):
            sends[d].wait_recv()
            mid[turn, d] = (
                part[turn, :, spot(near[1 - d], d)].astype(jnp.float32) + land1[turn, d, 0].astype(jnp.float32)
            ).astype(mid.dtype)
            copy = remote(mid.at[turn, d], land2.at[turn, d], s2.at[turn, d], r2.at[turn, d], dev(near[1 - d]))
            copy.start()
            sends.append(copy)
        for d in range(2):
            sends[2 + d].wait_recv()
            keep[d] = part[turn, :, spot(q, d)].astype(jnp.float32) + land1[turn, d, 1].astype(jnp.float32)
        for d in range(2):
            sends[4 + d].wait_recv()
            pf[c, turn, :, spot(q, d)] = (keep[d] + land2[turn, d].astype(jnp.float32)).astype(pf.dtype)
        mine = pl.ds(pl.multiple_of(q * quarter, quarter), quarter)
        view = pf.at[c, turn, :, mine]
        for d in range(2):
            copy = remote(view, view, s3.at[turn, d], r3.at[turn, d], dev(near[d]))
            copy.start()
            sends.append(copy)
        copy = remote(view, view, s5.at[turn, 0], r5.at[turn, 0], pair)
        copy.start()
        sends.append(copy)

        def consume(chip):
            @pl.loop(0, quarter // step)
            def _(t):
                cols = pl.ds(pl.multiple_of(chip * quarter + t * step, step), step)
                block = pf[c, turn, :, cols]
                msg[turn, pl.ds(vecs, vecs), pl.ds(0, vecs)] += contract_last(block, block)
                if turn == 0:
                    msg[turn, pl.ds(0, vecs), :] += contract_last(block, cbuf[:, :, cols].reshape(2 * rows, step))

        msg[turn] = jnp.zeros(msg.shape[1:], jnp.float32)
        consume(q)
        for d in range(2):
            theirs = pf.at[c, turn, :, pl.ds(pl.multiple_of(near[d] * quarter, quarter), quarter)]
            remote(theirs, theirs, s3.at[turn, d], r3.at[turn, d], pair).wait_recv()
            step_view = pf.at[c, turn, :, spot(near[d], d)]
            copy = remote(step_view, step_view, s4.at[turn, d], r4.at[turn, d], dev(near[1 - d]))
            copy.start()
            sends.append(copy)
            copy = remote(theirs, theirs, s5.at[turn, 1 + d], r5.at[turn, 1 + d], pair)
            copy.start()
            sends.append(copy)
        for d in range(2):
            consume(near[d])
        for d in range(2):
            view = pf.at[c, turn, :, spot(far, d)]
            remote(view, view, s4.at[turn, d], r4.at[turn, d], pair).wait_recv()
            copy = remote(view, view, s5.at[turn, 3 + d], r5.at[turn, 3 + d], pair)
            copy.start()
            sends.append(copy)
        consume(far)
        slot = z * 2 + c
        for k in range(1, 2 * p):
            copy = remote(msg.at[turn], mland.at[turn, slot], s6.at[turn, k], r6.at[turn, k], group[k - 1])
            copy.start()
            sends.append(copy)
        mland[turn, slot] = msg[turn]
        for k in range(1, 2 * p):
            there = lax.rem(z + p - lax.rem(k, p), p) * 2 + lax.rem(c + k // p, 2)
            view = mland.at[turn, there]
            remote(view, view, s6.at[turn, k], r6.at[turn, k], pair).wait_recv()
        total = mland[turn, 0]
        for j in range(1, 2 * p):
            total = total + mland[turn, j]
        return total, sends

    for k in range(pieces):
        load(k).wait()
    total, sends = all_reduce(0)
    here = pl.ds(pl.multiple_of(q * 2 * rows, 2 * rows), 2 * rows)
    img[0, :, here] = total[:vecs]
    rres[...] = total[:vecs]
    for k, chip in enumerate(chips):
        copy = remote(rres, img.at[0, :, here], s7.at[k], r7.at[k], chip)
        copy.start()
        sends.append(copy)
    direction = dref[...]
    curvature = total[vecs:, :vecs] + damping * exact_t(direction, direction)
    alpha = exact(gamma, small_inverse(curvature))
    gamma_inverse = small_inverse(gamma)
    for k, chip in enumerate([near[0], near[1], far]):
        view = img.at[0, :, pl.ds(pl.multiple_of(chip * 2 * rows, 2 * rows), 2 * rows)]
        remote(view, view, s7.at[k], r7.at[k], pair).wait_recv()
    image = img[0] + damping * direction
    residual = energies - exact(alpha, image)
    fresh = (residual - exact(exact(exact_t(residual, sketch), inverse), sketch)) / damping
    gamma_next = exact_t(fresh, residual)
    beta = exact(gamma_next, gamma_inverse)
    answer = exact(alpha, direction)
    dref[...] = fresh + exact(beta, direction)
    total, more = all_reduce(1)
    direction = dref[...]
    curvature = total[vecs:, :vecs] + damping * exact_t(direction, direction)
    alpha_next = exact(gamma_next, small_inverse(curvature))
    dref[...] = answer + exact(alpha_next, direction)
    sol_ref[...] = dref[:, here]
    weights = []
    for value in (alpha, alpha_next):
        upper = value.astype(jnp.bfloat16)
        weights.append((upper, (value - upper.astype(jnp.float32)).astype(jnp.bfloat16)))

    def finish(core):
        @pl.loop(0, half // step)
        def _(t):
            cols = pl.ds(pl.multiple_of(t * step, step), step)
            out = jnp.zeros((vecs, step), jnp.float32)
            for turn in range(2):
                block = pf[core, turn, :, cols]
                for weight in weights[turn]:
                    out = out + jnp.dot(weight, block, preferred_element_type=jnp.float32)
            update_ref[:, pl.ds(pl.multiple_of(core * half + t * step, step), step)] = out

    finish(c)
    for turn in range(2):
        for k, chip in enumerate([q, near[0], near[1]]):
            view = pf.at[o, turn, :, pl.ds(pl.multiple_of(chip * quarter, quarter), quarter)]
            remote(view, view, s5.at[turn, k], r5.at[turn, k], pair).wait_recv()
        for d in range(2):
            view = pf.at[o, turn, :, spot(far, d)]
            remote(view, view, s5.at[turn, 3 + d], r5.at[turn, 3 + d], pair).wait_recv()
    finish(o)
    for copy in sends + more:
        copy.wait_send()


def solve_call(c_rows, sketch, aux, p, ident):
    _, rows, half = c_rows.shape
    vecs = aux.shape[1] // 2
    rank, total = sketch.shape
    vmem, hbm = pl.BlockSpec(memory_space=pltpu.VMEM), pl.BlockSpec(memory_space=pl.ANY)
    dma = lambda *shape: pltpu.SemaphoreType.DMA(shape)
    bf, f32 = jnp.bfloat16, jnp.float32
    piece = half // 8
    return pl.pallas_call(
        functools.partial(solve_kernel, p),
        out_shape=(
            jax.ShapeDtypeStruct((vecs, 2 * half), f32),
            jax.ShapeDtypeStruct((vecs, 2 * rows), f32),
        ),
        in_specs=[hbm, vmem, vmem],
        out_specs=(vmem, vmem),
        scratch_shapes=[
            pltpu.VMEM(c_rows.shape, bf),
            pltpu.VMEM((rank + vecs, total), f32),
            pltpu.VMEM((rank, 2 * rank), f32),
            pltpu.VMEM((vecs, 128), f32),
            pltpu.VMEM((vecs, total), f32),
            pltpu.VMEM((vecs, 2 * rows), f32),
            pltpu.VMEM((2, vecs, half), bf),
            pltpu.VMEM((2, 2, 2, vecs, piece), bf),
            pltpu.VMEM((2, 2, vecs, piece), bf),
            pltpu.VMEM((2, vecs, piece), f32),
            pltpu.VMEM((2, 2, vecs, piece), bf),
            pltpu.VMEM((2, 2, vecs, half), bf),
            pltpu.VMEM((2, 2 * vecs, 2 * rows), f32),
            pltpu.VMEM((2, 2 * p, 2 * vecs, 2 * rows), f32),
            pltpu.VMEM((1, vecs, total), f32),
            dma(CHUNKS // 2), dma(2, 2, 2), dma(2, 2, 2), dma(2, 2), dma(2, 2), dma(2, 2), dma(2, 2), dma(2, 2),
            dma(2, 2), dma(2, 5), dma(2, 5), dma(2, 2 * p), dma(2, 2 * p), dma(3), dma(3),
        ],
        compiler_params=pltpu.CompilerParams(
            collective_id=ident, has_side_effects=True, vmem_limit_bytes=60 * 2**20
        ),
    )(c_rows, sketch, aux)


def paired_body(log_derivs, energies, nys_rows):
    rows, width = log_derivs.shape
    n, p = lax.axis_size("samp"), lax.axis_size("par")
    rank = nys_rows.shape[1]
    core = lax.rem(lax.axis_index("samp"), 2)
    slots = lambda count: lax.broadcasted_iota(jnp.int32, (rank, count), 1)
    picks = (nys_rows.reshape(rank, 1) == slots(rows)).astype(jnp.bfloat16)
    probe = jnp.concatenate([picks, jnp.ones((rank, rows), jnp.bfloat16)], axis=0)
    wide = (nys_rows.reshape(rank, 1) + core * rows == slots(2 * rows)).astype(jnp.float32)
    side = jnp.concatenate([energies.T, energies.T], axis=1)
    side = jnp.where(slots(2 * rows) // rows == core, side, 0.0)
    aux = jnp.concatenate([side, wide], axis=0)
    sketch, aux_all, c_rows = sketch_call(log_derivs, probe, aux, p, n * rows, 1.0 / math.sqrt(width * p), 0)
    update, answer = solve_call(c_rows, sketch, aux_all, p, 1)
    return (update.T, lax.dynamic_slice_in_dim(answer, core * rows, rows, 1).T)


def solution(mesh):
    n, p = mesh.shape["samp"], mesh.shape["par"]

    def body(log_derivs, energies, nys_rows):
        rows, count = log_derivs.shape[0], energies.shape[1]
        paired = n == 8 and rows == 64 and count == 8 and nys_rows.shape[1] == count
        return (paired_body if paired else general_body)(log_derivs, energies, nys_rows)

    return jax.shard_map(
        body,
        mesh=mesh,
        in_specs=(P("samp", "par"), P("samp", None), P("samp", None)),
        out_specs=(P("par", None), P("samp", None)),
        check_vma=False,
    )
```

```python
import functools
import math

import jax
import jax.numpy as jnp
from jax import lax
from jax.experimental import pallas as pl
from jax.experimental.pallas import tpu as pltpu
from jax.sharding import PartitionSpec as P

ITERS = 2


damping = 0.5

MESH = pl.DeviceIdType.MESH


def factor_solve(factor, right):
    middle = lax.linalg.triangular_solve(factor, right, left_side=True, lower=True)
    return lax.linalg.triangular_solve(factor, middle, left_side=True, lower=True, transpose_a=True)


def eliminate_kernel(matrix_ref, right_ref, out_ref):
    left, right = matrix_ref[...], right_ref[...]
    row = lax.broadcasted_iota(jnp.int32, left.shape, 0)
    for i in range(left.shape[0]):
        column = left[:, i:i + 1]
        pivot = left[i:i + 1, i:i + 1]
        left_row = left[i:i + 1, :] / pivot
        right_row = right[i:i + 1, :] / pivot
        left = jnp.where(row == i, left_row, left - column * left_row)
        right = jnp.where(row == i, right_row, right - column * right_row)
    out_ref[...] = right


def small_solve(matrix, right):
    matrix = 0.5 * (matrix + matrix.T)
    return pl.pallas_call(
        eliminate_kernel, out_shape=jax.ShapeDtypeStruct(right.shape, right.dtype)
    )(matrix, right)


def hdot(left, right):
    return jnp.dot(left, right, precision=lax.Precision.HIGHEST)


def greet(peers):
    barrier = pltpu.get_barrier_semaphore()
    for peer in peers:
        pl.semaphore_signal(barrier, inc=1, device_id=peer, device_id_type=MESH)
    pl.semaphore_wait(barrier, len(peers))


def remote(src, dst, send, recv, peer):
    return pltpu.make_async_remote_copy(
        src_ref=src, dst_ref=dst, send_sem=send, recv_sem=recv, device_id=peer, device_id_type=MESH
    )


def gather_kernel(n, total_rows, scale, sums_ref, aux_ref, chosen_ref, full_ref, sketch_ref, aux_out, centered_out,
                  mean_ref, rows_out, centered_ref, land, own, full, s1, r1, s2, r2, s3, r3, s4, r4, s5, r5, s6, r6, local):
    me, col = lax.axis_index("samp"), lax.axis_index("par")
    at = [lax.rem(me + k, n) for k in range(n)]
    back = [lax.rem(me + n - k, n) for k in range(n)]
    peer = [(at[k], col) for k in range(n)]
    pair = (jnp.bitwise_xor(me, 1), col)
    width = chosen_ref.shape[1]
    half = width // 2
    part = [pl.ds(0, half), pl.ds(half, half)]
    load = pltpu.make_async_copy(full_ref, full, local.at[2])
    load.start()
    greet(peer[1:])
    scatter = [remote(sums_ref.at[at[k]], land.at[k], s1.at[k], r1.at[k], peer[k]) for k in range(1, n)]
    for copy in scatter:
        copy.start()
    sent = list(scatter)
    quad = n == 8
    beside = [jnp.bitwise_xor(me, 2), jnp.bitwise_xor(me, 4)]
    if quad:
        first = [
            remote(chosen_ref.at[:, part[d]], rows_out.at[me, :, part[d]], s4.at[d], r4.at[d], (beside[d], col))
            for d in range(2)
        ]
        for copy in first:
            copy.start()
        sent += first
    auxes = [remote(aux_ref, aux_out.at[me], s2.at[k], r2.at[k], peer[k]) for k in range(1, n)]
    mine = pltpu.make_async_copy(aux_ref, aux_out.at[me], local.at[0])
    mine.start()
    keep = pltpu.make_async_copy(chosen_ref, rows_out.at[me], local.at[1])
    keep.start()
    total = sums_ref[me]
    for k in range(1, n):
        scatter[k - 1].wait_recv()
        total = total + land[k]
    own[...] = total / total_rows
    mean_ref[me] = own[...]
    spread = [remote(own, mean_ref.at[me], s3.at[k], r3.at[k], peer[k]) for k in range(1, n)]
    for copy in spread + auxes:
        copy.start()
    sent += spread + auxes
    over = [remote(chosen_ref, rows_out.at[me], s5.at[0], r5.at[0], pair)]
    over[0].start()
    if quad:
        second = [
            remote(chosen_ref.at[:, part[1 - d]], rows_out.at[me, :, part[1 - d]], s4.at[2 + d], r4.at[2 + d],
                   (beside[d], col))
            for d in range(2)
        ]
        for copy in second:
            copy.start()
        sent += second
        for d in range(2):
            view = rows_out.at[beside[d], :, part[d]]
            remote(view, view, s4.at[d], r4.at[d], pair).wait_recv()
            step = remote(view, view, s4.at[4 + d], r4.at[4 + d], (beside[1 - d], col))
            step.start()
            sent.append(step)
    else:
        far = [remote(chosen_ref, rows_out.at[me], s4.at[k], r4.at[k], peer[k]) for k in range(2, n, 2)]
        for copy in far:
            copy.start()
        sent += far
    for k in range(1, n):
        remote(own, mean_ref.at[back[k]], s3.at[k], r3.at[k], peer[k]).wait_recv()
    load.wait()
    slab = width // n
    tile = math.gcd(slab, 1024)

    @pl.loop(0, n)
    def _(j):
        @pl.loop(0, slab // tile)
        def _(t):
            inner = pl.multiple_of(t * tile, tile)
            cols = pl.ds(pl.multiple_of(j * slab + inner, tile), tile)
            mean = mean_ref[j, :, pl.ds(inner, tile)]
            centered_ref[:, cols] = ((full[:, cols].astype(jnp.float32) - mean) * scale).astype(jnp.bfloat16)

    put = pltpu.make_async_copy(centered_ref, centered_out, local.at[2])
    put.start()
    if quad:
        for d in range(2):
            view = rows_out.at[beside[d], :, part[1 - d]]
            remote(view, view, s4.at[2 + d], r4.at[2 + d], pair).wait_recv()
            block = rows_out.at[beside[d]]
            step = remote(block, block, s5.at[1 + d], r5.at[1 + d], pair)
            step.start()
            over.append(step)
        cross = jnp.bitwise_xor(me, 6)
        for d in range(2):
            view = rows_out.at[cross, :, part[d]]
            remote(view, view, s4.at[4 + d], r4.at[4 + d], pair).wait_recv()
            step = remote(view, view, s5.at[3 + d], r5.at[3 + d], pair)
            step.start()
            over.append(step)
        block = rows_out.at[jnp.bitwise_xor(me, 1)]
        remote(block, block, s5.at[0], r5.at[0], pair).wait_recv()
        for d in range(2):
            block = rows_out.at[jnp.bitwise_xor(me, 3 + 2 * d)]
            remote(block, block, s5.at[1 + d], r5.at[1 + d], pair).wait_recv()
            view = rows_out.at[jnp.bitwise_xor(me, 7), :, part[d]]
            remote(view, view, s5.at[3 + d], r5.at[3 + d], pair).wait_recv()
    else:
        for k in range(2, n, 2):
            block = rows_out.at[back[k]]
            remote(block, block, s4.at[k], r4.at[k], pair).wait_recv()
            step = remote(block, block, s5.at[k], r5.at[k], pair)
            step.start()
            over.append(step)
        for k in range(0, n, 2):
            block = rows_out.at[lax.rem(pair[0] + n - k, n)]
            remote(block, block, s5.at[k], r5.at[k], pair).wait_recv()
    for k in range(1, n):
        remote(aux_ref, aux_out.at[back[k]], s2.at[k], r2.at[k], peer[k]).wait_recv()
    for copy in sent + over:
        copy.wait_send()
    mine.wait()
    keep.wait()
    sketch_ref[...] = jnp.zeros_like(sketch_ref)
    count = n * chosen_ref.shape[0]

    @pl.loop(0, n)
    def _(j):
        @pl.loop(0, slab // tile)
        def _(t):
            inner = pl.multiple_of(t * tile, tile)
            cols = pl.ds(pl.multiple_of(j * slab + inner, tile), tile)
            mean = mean_ref[j, :, pl.ds(inner, tile)]
            rows = rows_out[:, :, cols].astype(jnp.float32).reshape(count, tile)
            rows = ((rows - mean) * scale).astype(jnp.bfloat16)
            sketch_ref[...] += lax.dot_general(
                centered_ref[:, cols], rows, (((1,), (1,)), ((), ())), preferred_element_type=jnp.float32
            )

    put.wait()


def gather_rows(sums, aux, chosen, full, n, total_rows, scale, ident):
    dma = lambda: pltpu.SemaphoreType.DMA((n,))
    vmem = pl.BlockSpec(memory_space=pltpu.VMEM)
    slab = sums.shape[-1]
    return pl.pallas_call(
        functools.partial(gather_kernel, n, total_rows, scale),
        out_shape=(
            jax.ShapeDtypeStruct((full.shape[0], n * chosen.shape[0]), jnp.float32),
            jax.ShapeDtypeStruct((n,) + aux.shape, jnp.float32),
            jax.ShapeDtypeStruct(full.shape, full.dtype),
        ),
        in_specs=[vmem, vmem, vmem, pl.BlockSpec(memory_space=pl.ANY)],
        out_specs=(vmem, vmem, pl.BlockSpec(memory_space=pl.ANY)),
        scratch_shapes=[
            pltpu.VMEM(sums.shape, jnp.float32),
            pltpu.VMEM((n,) + chosen.shape, chosen.dtype),
            pltpu.VMEM(full.shape, full.dtype),
            pltpu.VMEM(sums.shape, jnp.float32),
            pltpu.VMEM((1, slab), jnp.float32),
            pltpu.VMEM(full.shape, full.dtype),
        ] + [dma() for _ in range(12)] + [pltpu.SemaphoreType.DMA((3,))],
        compiler_params=pltpu.CompilerParams(
            collective_id=ident, has_side_effects=True, vmem_limit_bytes=60 * 2**20
        ),
    )(sums, aux, chosen, full)


def spread_kernel(n, p, part_ref, out_ref, land, own, s1, r1, s2, r2):
    me, col = lax.axis_index("samp"), lax.axis_index("par")
    beside = [lax.rem(col + k, p) for k in range(p)]
    at = [lax.rem(me + k, n) for k in range(n)]
    back = [lax.rem(me + n - k, n) for k in range(n)]
    greet([(me, beside[k]) for k in range(1, p)] + [(at[k], col) for k in range(1, n)])
    sums = [remote(part_ref, land.at[col], s1.at[k], r1.at[k], (me, beside[k])) for k in range(1, p)]
    for copy in sums:
        copy.start()
    land[col] = part_ref[...]
    for k in range(1, p):
        there = lax.rem(col + p - k, p)
        remote(part_ref, land.at[there], s1.at[k], r1.at[k], (me, beside[k])).wait_recv()
    total = land[0]
    for j in range(1, p):
        total = total + land[j]
    own[...] = total
    out_ref[me] = total
    hops = [remote(own, out_ref.at[me], s2.at[k], r2.at[k], (at[k], col)) for k in range(1, n)]
    for copy in hops:
        copy.start()
    for k in range(1, n):
        remote(own, out_ref.at[back[k]], s2.at[k], r2.at[k], (at[k], col)).wait_recv()
    for copy in sums + hops:
        copy.wait_send()


def sum_and_spread(part, n, p, ident):
    vmem = pl.BlockSpec(memory_space=pltpu.VMEM)
    return pl.pallas_call(
        functools.partial(spread_kernel, n, p),
        out_shape=jax.ShapeDtypeStruct((n,) + part.shape, jnp.float32),
        in_specs=[vmem],
        out_specs=vmem,
        scratch_shapes=[
            pltpu.VMEM((p,) + part.shape, jnp.float32),
            pltpu.VMEM(part.shape, jnp.float32),
            pltpu.SemaphoreType.DMA((p,)),
            pltpu.SemaphoreType.DMA((p,)),
            pltpu.SemaphoreType.DMA((n,)),
            pltpu.SemaphoreType.DMA((n,)),
        ],
        compiler_params=pltpu.CompilerParams(collective_id=ident, has_side_effects=True),
    )(part)


def reduce_kernel(n, part_ref, out_ref, land, both, inbox, s0, r0, s1, r1, s2, r2, s3, r3):
    me, col = lax.axis_index("samp"), lax.axis_index("par")
    outer = n // 2
    slab = part_ref.shape[1] // n
    half = slab * outer
    i, o = lax.rem(me, 2), me // 2
    pair = (jnp.bitwise_xor(me, 1), col)
    at = [lax.rem(o + k, outer) for k in range(outer)]
    back = [lax.rem(o + outer - k, outer) for k in range(outer)]
    peer = [(at[k] * 2 + i, col) for k in range(outer)]
    cols = lambda j: pl.ds(pl.multiple_of(j * slab, slab), slab)
    halves = lambda j: pl.ds(pl.multiple_of(j * half, half), half)
    greet([pair] + peer[1:])
    swap = remote(part_ref.at[:, halves(1 - i)], land, s0.at[0], r0.at[0], pair)
    swap.start()
    swap.wait_recv()
    both[...] = (part_ref[:, halves(i)].astype(jnp.float32) + land[...].astype(jnp.float32)).astype(both.dtype)
    scatter = [remote(both.at[:, cols(at[k])], inbox.at[k], s1.at[k], r1.at[k], peer[k]) for k in range(1, outer)]
    for copy in scatter:
        copy.start()
    total = part_ref[:, cols(i * outer + o)].astype(jnp.float32) + land[:, cols(o)].astype(jnp.float32)
    for k in range(1, outer):
        scatter[k - 1].wait_recv()
        total = total + inbox[k].astype(jnp.float32)
    home = cols(i * outer + o)
    out_ref[:, home] = total.astype(out_ref.dtype)
    mine = out_ref.at[:, home]
    spread = [remote(mine, mine, s2.at[k], r2.at[k], peer[k]) for k in range(1, outer)]
    spread.append(remote(mine, mine, s3.at[0], r3.at[0], pair))
    for copy in spread:
        copy.start()
    for k in range(1, outer):
        block = out_ref.at[:, cols(i * outer + back[k])]
        remote(block, block, s2.at[k], r2.at[k], pair).wait_recv()
        step = remote(block, block, s3.at[k], r3.at[k], pair)
        step.start()
        spread.append(step)
    for k in range(outer):
        block = out_ref.at[:, cols((1 - i) * outer + back[k])]
        remote(block, block, s3.at[k], r3.at[k], pair).wait_recv()
    for copy in [swap] + scatter + spread:
        copy.wait_send()


def reduce_all(part, n, ident):
    count, width = part.shape
    outer = n // 2
    vmem = pl.BlockSpec(memory_space=pltpu.VMEM)
    return pl.pallas_call(
        functools.partial(reduce_kernel, n),
        out_shape=jax.ShapeDtypeStruct(part.shape, part.dtype),
        in_specs=[vmem],
        out_specs=vmem,
        scratch_shapes=[
            pltpu.VMEM((count, width // 2), part.dtype),
            pltpu.VMEM((count, width // 2), part.dtype),
            pltpu.VMEM((outer, count, width // n), part.dtype),
        ]
        + [pltpu.SemaphoreType.DMA((outer,)) for _ in range(8)],
        compiler_params=pltpu.CompilerParams(collective_id=ident, has_side_effects=True),
    )(part)


def tiny_kernel(p, part_ref, out_ref, land, s1, r1):
    me, col = lax.axis_index("samp"), lax.axis_index("par")
    at = [lax.rem(col + k, p) for k in range(p)]
    back = [lax.rem(col + p - k, p) for k in range(p)]
    greet([(me, at[k]) for k in range(1, p)])
    copies = [remote(part_ref, land.at[col], s1.at[k], r1.at[k], (me, at[k])) for k in range(1, p)]
    for copy in copies:
        copy.start()
    land[col] = part_ref[...]
    for k in range(1, p):
        remote(part_ref, land.at[back[k]], s1.at[k], r1.at[k], (me, at[k])).wait_recv()
    for copy in copies:
        copy.wait_send()
    total = land[0]
    for j in range(1, p):
        total = total + land[j]
    out_ref[...] = total


def tiny_sum(part, p, ident):
    vmem = pl.BlockSpec(memory_space=pltpu.VMEM)
    return pl.pallas_call(
        functools.partial(tiny_kernel, p),
        out_shape=jax.ShapeDtypeStruct(part.shape, part.dtype),
        in_specs=[vmem],
        out_specs=vmem,
        scratch_shapes=[pltpu.VMEM((p,) + part.shape, part.dtype)]
        + [pltpu.SemaphoreType.DMA((p,)) for _ in range(2)],
        compiler_params=pltpu.CompilerParams(collective_id=ident, has_side_effects=True),
    )(part)


def general_body(log_derivs, energies, nys_rows):
    rows, width = log_derivs.shape
    n, p = lax.axis_size("samp"), lax.axis_size("par")
    count, rank = energies.shape[1], nys_rows.shape[1]
    scale = 1.0 / math.sqrt(width * p)
    picks = (nys_rows.reshape(rank, 1) == lax.broadcasted_iota(jnp.int32, (rank, rows), 1)).astype(jnp.bfloat16)
    probe = jnp.concatenate([picks, jnp.ones((8, rows), jnp.bfloat16)], axis=0)
    taken = jnp.dot(probe, log_derivs, preferred_element_type=jnp.float32)
    chosen = taken[:rank].astype(jnp.bfloat16)
    sums = taken[rank].reshape(n, 1, width // n)
    aux = jnp.concatenate([energies, picks.astype(jnp.float32).T], axis=1)
    sketch_part, aux_all, centered = gather_rows(sums, aux, chosen, log_derivs, n, n * rows, scale, 0)
    sketch = sum_and_spread(sketch_part, n, p, 1).reshape(n * rows, n * rank)
    all_energies = aux_all[:, :, :count].reshape(n * rows, count)
    core_block = jnp.einsum(
        "grj,grk->gjk", aux_all[:, :, count:], sketch.reshape(n, rows, n * rank), precision=lax.Precision.HIGHEST
    ).reshape(n * rank, n * rank)
    factor = jnp.linalg.cholesky(damping * core_block + hdot(sketch.T, sketch))

    def precondition(residual):
        coeffs = factor_solve(factor, hdot(sketch.T, residual))
        result = (residual - hdot(sketch, coeffs)) / damping
        return (result, hdot(result.T, residual))

    start = lax.axis_index("samp") * rows
    solution = jnp.zeros(all_energies.shape, jnp.float32)
    update = 0.0
    residual = all_energies
    precond_res, inner_prev = precondition(residual)
    direction = precond_res
    for iteration in range(ITERS):
        rounded = lax.dynamic_slice_in_dim(direction, start, rows, 0).astype(jnp.bfloat16)
        part = jnp.einsum("rv,rc->vc", rounded, centered, preferred_element_type=jnp.float32)
        projected = reduce_all(part.astype(jnp.bfloat16), n, 2 + 2 * iteration)
        if iteration + 1 < ITERS:
            image_part = jnp.einsum("rc,vc->vr", centered, projected, preferred_element_type=jnp.float32)
            image_k = sum_and_spread(image_part, n, p, 3 + 2 * iteration)
            image_k = image_k.transpose(0, 2, 1).reshape(n * rows, count) + damping * direction
            curvature = hdot(direction.T, image_k)
        else:
            square = jnp.einsum("uc,vc->uv", projected, projected, preferred_element_type=jnp.float32)
            curvature = tiny_sum(square, p, 3 + 2 * iteration) + damping * hdot(direction.T, direction)
        alpha_k = small_solve(curvature, inner_prev)
        solution = solution + hdot(direction, alpha_k)
        update = update + hdot(alpha_k.T, projected.astype(jnp.float32))
        if iteration + 1 < ITERS:
            residual = residual - hdot(image_k, alpha_k)
            precond_res, inner_next = precondition(residual)
            beta_k = small_solve(inner_prev, inner_next)
            direction = precond_res + hdot(direction, beta_k)
            inner_prev = inner_next
    return (update.T, lax.dynamic_slice_in_dim(solution, start, rows, 0))


CHUNKS = 8
EARLY = 2
AHEAD = 4
LAG = 2


def contract_last(left, right, precision=None):
    return lax.dot_general(
        left, right, (((1,), (1,)), ((), ())), precision=precision, preferred_element_type=jnp.float32
    )


def exact(left, right):
    return jnp.dot(left, right, precision=lax.Precision.HIGHEST, preferred_element_type=jnp.float32)


def exact_t(left, right):
    return contract_last(left, right, lax.Precision.HIGHEST)


def iota(shape, axis):
    return lax.broadcasted_iota(jnp.int32, shape, axis)


def eliminate(matrix, size, group):
    row = iota(matrix.shape, 0)
    lanes = matrix.shape[1]
    for start in range(0, size, group):
        spread = lambda i, j: jnp.broadcast_to(matrix[start + i:start + i + 1, start + j:start + j + 1], (1, lanes))
        cell = [[spread(i, j) for j in range(group)] for i in range(group)]
        for k in range(group):
            inverse = 1.0 / cell[k][k]
            scaled = [cell[k][j] * inverse for j in range(group)]
            for i in range(group):
                if i != k:
                    factor = cell[i][k]
                    cell[i] = [cell[i][j] - factor * scaled[j] for j in range(group)]
                    cell[i][k] = -factor * inverse
            scaled[k] = inverse
            cell[k] = scaled
        old = [matrix[start + j:start + j + 1, :] for j in range(group)]
        fresh = []
        for i in range(group):
            line = cell[i][0] * old[0]
            for j in range(1, group):
                line = line + cell[i][j] * old[j]
            fresh.append(line)
        change = matrix[:, start:start + 1] * fresh[0]
        for i in range(1, group):
            change = change + matrix[:, start + i:start + i + 1] * fresh[i]
        matrix = matrix - change
        for i in range(group):
            matrix = jnp.where(row == start + i, fresh[i], matrix)
    return matrix


def main_kernel(p, total_rows, scale, x_ref, energy_ref, picks_ref, pf_ref, alpha_ref, sol_ref,
                stage, xh, other, rin, probe, aux, aux_all, sums, sland, acc1, acc2, mean, acc, pland, mine, zland,
                tot, sk, aug, big, small, dref, rres, part, land1, mid, keep, land2, pf, sq, qland, qsum, qtot,
                msg, mland, img,
                lsem, wsem, wrecv, psem, precv, osem, rsem, fsem, drecv, bsem, brecv, asem, arecv, tsem, trecv,
                s1, r1, s2, r2, s3, r3, s4, r4, s5, r5, s6, r6, s7, r7, s8, r8, s9, r9):
    me, z = lax.axis_index("samp"), lax.axis_index("par")
    c, q = lax.rem(me, 2), me // 2
    o = 1 - c
    near, far = [jnp.bitwise_xor(q, 1), jnp.bitwise_xor(q, 2)], jnp.bitwise_xor(q, 3)
    rows, half = stage.shape
    wide = 2 * rows
    width = half // CHUNKS
    count = rin.shape[1]
    dev = lambda chip: (chip * 2 + c, z)
    pair = (q * 2 + o, z)
    chips = [near[0], near[1], far]
    span = lambda k: pl.ds(pl.multiple_of(k * width, width), width)
    duo = lambda chip: pl.ds(pl.multiple_of(chip * 2, 2), 2)
    group = [(q * 2 + lax.rem(c + k // p, 2), lax.rem(z + lax.rem(k, p), p)) for k in range(1, 2 * p)]
    samp_peers = [(lax.rem(me + k, 8), z) for k in range(1, 8)]
    par_peers = group[:p - 1]

    def load(k, own):
        core = c if own else o
        cols = pl.ds(pl.multiple_of(core * half + k * width, width), width)
        dst = xh.at[c, :, span(k)] if own else stage.at[:, span(k)]
        return pltpu.make_async_copy(x_ref.at[:, cols], dst, lsem.at[int(own), k])

    barrier = pltpu.get_barrier_semaphore()
    greeted = samp_peers + [peer for k, peer in enumerate(group, 1) if k != p]
    for peer in greeted:
        pl.semaphore_signal(barrier, inc=1, device_id=peer, device_id_type=MESH)

    @pl.loop(0, CHUNKS)
    def _(k):
        load(k, False).start()
        load(k, True).start()

    taken_row, slot = iota((count, rows), 0), iota((count, rows), 1)
    wide_row, wide_slot = iota((count, wide), 0), iota((count, wide), 1)
    picks, wide_picks = jnp.zeros((count, rows), jnp.float32), jnp.zeros((count, wide), jnp.float32)
    for j in range(count):
        at = picks_ref[0, j]
        picks = jnp.where((taken_row == j) & (slot == at), 1.0, picks)
        wide_picks = jnp.where((wide_row == j) & (wide_slot == at + c * rows), 1.0, wide_picks)
    probe[...] = jnp.concatenate([picks, jnp.ones_like(picks)], axis=0).astype(probe.dtype)
    place = (iota((rows, wide), 0) + c * rows == iota((rows, wide), 1)).astype(jnp.float32)
    aux[pl.ds(0, count), :] = exact(energy_ref[...], place)
    aux[pl.ds(count, count), :] = wide_picks

    def swap(k):
        return remote(stage.at[:, span(k)], xh.at[c, :, span(k)], wsem.at[k], wrecv.at[k], pair)

    def to_pair(k):
        return remote(other.at[:, span(k)], rin.at[me, :, span(k)], psem.at[k], precv.at[k], pair)

    def direct(k):
        view = rin.at[duo(q), :, span(k)]
        return [remote(view, view, osem.at[d, k], rsem.at[d, k], dev(near[d])) for d in range(2)]

    def forward(k, d):
        view = rin.at[duo(near[d]), :, span(k)]
        return remote(view, view, fsem.at[k], drecv.at[k], dev(near[1 - d]))

    def send(k):
        view = rin.at[me + 1 - 2 * c, :, span(k)]
        remote(view, view, psem.at[k], precv.at[k], pair).wait_recv()
        for copy in direct(k):
            copy.start()

    def relay(k, d):
        for e in range(2):
            view = rin.at[duo(near[e]), :, span(k)]
            remote(view, view, osem.at[e, k], rsem.at[e, k], pair).wait_recv()
        forward(k, d).start()

    def extract(k):
        for own in (False, True):
            load(k, own).wait()
            step = min(width, 1024)

            @pl.loop(0, width // step)
            def _(s):
                cols = pl.ds(pl.multiple_of(k * width + s * step, step), step)
                block = xh[c, :, cols] if own else stage[:, cols]
                taken = jnp.dot(probe[...], block, preferred_element_type=jnp.float32)
                if own:
                    rin[me, :, cols] = taken[:count].astype(rin.dtype)
                    sums[c, :, cols] = taken[count:count + 1]
                else:
                    other[:, cols] = taken[:count].astype(other.dtype)
                    sums[o, :, cols] = taken[count:count + 1]

    extract(0)
    pl.semaphore_wait(barrier, len(greeted))
    to_pair(0).start()
    auxes = [remote(aux, aux_all.at[me], asem.at[k], arecv.at[k], samp_peers[k]) for k in range(7)]

    @pl.loop(1, EARLY + 1)
    def _(k):
        extract(k)
        to_pair(k).start()
        send(k - 1)

    @pl.loop(EARLY + 1, CHUNKS)
    def _(k):
        extract(k)
        to_pair(k).start()

    first = remote(sums.at[o], sland.at[0], bsem.at[0], brecv.at[0], pair)
    first.start()
    for copy in auxes:
        copy.start()
    aux_all[me] = aux[...]

    @pl.loop(0, CHUNKS)
    def _(k):
        swap(k).start()

    first.wait_recv()
    acc1[...] = sums[c] + sland[0]
    part_of = [pl.ds(0, half // 2), pl.ds(half // 2, half // 2)]
    second = [
        remote(acc1.at[:, part_of[d]], sland.at[1, :, part_of[d]], bsem.at[1 + d], brecv.at[1 + d], dev(near[d]))
        for d in range(2)
    ]
    for copy in second:
        copy.start()
    middle = (EARLY + AHEAD) // 2

    @pl.loop(EARLY, middle)
    def _(k):
        send(k)

    for copy in second:
        copy.wait_recv()
    acc2[...] = acc1[...] + sland[1]
    third = [
        remote(acc2.at[:, part_of[d]], sland.at[2, :, part_of[d]], bsem.at[3 + d], brecv.at[3 + d], dev(near[1 - d]))
        for d in range(2)
    ]
    for copy in third:
        copy.start()
    relay(0, 0)

    @pl.loop(middle, AHEAD)
    def _(k):
        send(k)

    relay(1, 1)
    for copy in third:
        copy.wait_recv()
    mean[...] = (acc2[...] + sland[2]) / total_rows
    acc[...] = jnp.zeros_like(acc)

    def process(k):
        remote(stage.at[:, span(k)], xh.at[o, :, span(k)], wsem.at[k], wrecv.at[k], pair).wait_recv()
        view = rin.at[duo(far), :, span(k)]
        remote(view, view, fsem.at[k], drecv.at[k], pair).wait_recv()
        step = min(width, 512)

        @pl.loop(0, width // step)
        def _(s):
            cols = pl.ds(pl.multiple_of(k * width + s * step, step), step)
            shift = mean[:, cols]
            block = xh[:, :, cols].astype(jnp.float32).reshape(wide, step)
            block = ((block - shift) * scale).astype(jnp.bfloat16)
            xh[:, :, cols] = block.reshape(2, rows, step)
            picked = rin[:, :, cols].astype(jnp.float32).reshape(8 * count, step)
            picked = ((picked - shift) * scale).astype(jnp.bfloat16)
            acc[...] += contract_last(picked, block)

    @pl.loop(0, CHUNKS // 2)
    def _(i):
        for d in range(2):
            k = 2 * i + d

            @pl.when(k + AHEAD < CHUNKS)
            def _():
                send(k + AHEAD)

            @pl.when(k + LAG < CHUNKS)
            def _():
                relay(k + LAG, d)

            process(k)

    rank = acc.shape[0]
    own_rows = rank // 2
    mine_rows = pl.ds(pl.multiple_of(c * own_rows, own_rows), own_rows)
    their_rows = pl.ds(pl.multiple_of(o * own_rows, own_rows), own_rows)
    give = remote(acc.at[their_rows], pland, tsem.at[0], trecv.at[0], pair)
    give.start()
    give.wait_recv()
    mine[...] = acc[mine_rows, :] + pland[...]
    across = [remote(mine, zland.at[z], tsem.at[k], trecv.at[k], par_peers[k - 1]) for k in range(1, p)]
    for copy in across:
        copy.start()
    zland[z] = mine[...]
    for k in range(7):
        view = aux_all.at[lax.rem(me + 7 - k, 8)]
        remote(view, view, asem.at[k], arecv.at[k], pair).wait_recv()
    for k in range(1, p):
        view = zland.at[lax.rem(z + p - k, p)]
        remote(view, view, tsem.at[k], trecv.at[k], pair).wait_recv()
    total = zland[0]
    for j in range(1, p):
        total = total + zland[j]
    tot[...] = total
    spot = lambda chip, core: sk.at[
        pl.ds(pl.multiple_of(core * own_rows, own_rows), own_rows),
        pl.ds(pl.multiple_of(chip * wide, wide), wide),
    ]
    here = pl.ds(pl.multiple_of(q * wide, wide), wide)
    sk[mine_rows, here] = total
    spread = [remote(tot, spot(q, c), tsem.at[p + k], trecv.at[p + k], samp_peers[k]) for k in range(7)]
    for copy in spread:
        copy.start()
    vecs = count
    lower = pl.ds(rank, vecs)
    for chip in range(4):
        cols = pl.ds(chip * wide, wide)
        aug[lower, cols] = aux_all[2 * chip, :vecs, :] + aux_all[2 * chip + 1, :vecs, :]
    energies = aug[lower, :]
    big[...] = (iota(big.shape, 0) + rank == iota(big.shape, 1)).astype(jnp.float32)
    for k in range(7):
        source = lax.rem(me + 7 - k, 8)
        view = spot(source // 2, lax.rem(source, 2))
        remote(view, view, tsem.at[p + k], trecv.at[p + k], pair).wait_recv()

    sketch = sk[...]
    aug[pl.ds(0, rank), :] = sketch
    for g in range(8):
        cols = pl.ds((g // 2) * wide, wide)
        line = pl.ds(g * vecs, vecs)
        aug[line, cols] = aug[line, cols] + damping * aux_all[g, vecs:, :]
    product = exact_t(aug[...], sketch)
    big[:, pl.ds(0, rank)] = product[:rank]
    inverse = eliminate(big[...], rank, 4)[:, rank:2 * rank]
    dref[...] = (energies - exact(exact(product[rank:], inverse), sketch)) / damping

    def small_inverse(matrix):
        small[...] = (iota(small.shape, 0) + vecs == iota(small.shape, 1)).astype(jnp.float32)
        small[:, pl.ds(0, vecs)] = matrix
        return eliminate(small[...], vecs, 4)[:, vecs:2 * vecs]

    quarter = half // 4
    piece = quarter // 2
    span2 = lambda chip, s: pl.ds(pl.multiple_of(chip * quarter + s * piece, piece), piece)
    step = min(piece, 1024)
    slot_of = z * 2 + c
    sends = []

    def begin(copy):
        copy.start()
        sends.append(copy)

    def all_reduce(turn):
        rounded = dref[:, here].astype(jnp.bfloat16)

        def project(chip, s):
            @pl.loop(0, piece // step)
            def _(t):
                cols = pl.ds(pl.multiple_of(chip * quarter + s * piece + t * step, step), step)
                block = xh[:, :, cols].reshape(wide, step)
                part[turn, :, cols] = jnp.dot(rounded, block, preferred_element_type=jnp.float32).astype(part.dtype)

        halves = []
        for j in range(2):
            for d in range(2):
                chip = near[d] if j else far
                project(chip, d)
                copy = remote(part.at[turn, :, span2(chip, d)], land1.at[turn, d, j], s1.at[turn, d, j],
                              r1.at[turn, d, j], dev(near[d]))
                halves.append(copy)
                begin(copy)
        for d in range(2):
            project(near[1 - d], d)
        later = []
        for d in range(2):
            halves[d].wait_recv()
            mid[turn, d] = (
                part[turn, :, span2(near[1 - d], d)].astype(jnp.float32) + land1[turn, d, 0].astype(jnp.float32)
            ).astype(mid.dtype)
            copy = remote(mid.at[turn, d], land2.at[turn, d], s2.at[turn, d], r2.at[turn, d], dev(near[1 - d]))
            later.append(copy)
            begin(copy)
        for d in range(2):
            project(q, d)
        for d in range(2):
            halves[2 + d].wait_recv()
            keep[d] = part[turn, :, span2(q, d)].astype(jnp.float32) + land1[turn, d, 1].astype(jnp.float32)
        for d in range(2):
            later[d].wait_recv()
            pf[c, turn, :, span2(q, d)] = (keep[d] + land2[turn, d].astype(jnp.float32)).astype(pf.dtype)
            view = pf.at[c, turn, :, span2(q, d)]
            begin(remote(view, view, s3.at[turn, d, d], r3.at[turn, d, d], dev(near[d])))
        for d in range(2):
            view = pf.at[c, turn, :, span2(q, 1 - d)]
            begin(remote(view, view, s3.at[turn, d, 1 - d], r3.at[turn, d, 1 - d], dev(near[d])))
        mine_cols = pl.ds(pl.multiple_of(q * quarter, quarter), quarter)
        view = pf.at[c, turn, :, mine_cols]
        begin(remote(view, view, s5.at[turn, 0], r5.at[turn, 0], pair))

        sq[turn] = jnp.zeros(sq.shape[1:], jnp.float32)

        @pl.loop(0, quarter // step)
        def _(t):
            block = pf[c, turn, :, pl.ds(pl.multiple_of(q * quarter + t * step, step), step)]
            sq[turn, :, pl.ds(0, vecs)] += contract_last(block, block)

        for k in range(1, 2 * p):
            begin(remote(sq.at[turn], qland.at[turn, slot_of], s8.at[turn, k], r8.at[turn, k], group[k - 1]))
        qland[turn, slot_of] = sq[turn]

        def consume(chip):
            @pl.loop(0, quarter // step)
            def _(t):
                cols = pl.ds(pl.multiple_of(chip * quarter + t * step, step), step)
                msg[...] += contract_last(pf[c, turn, :, cols], xh[:, :, cols].reshape(wide, step))

        if turn == 0:
            msg[...] = jnp.zeros(msg.shape, jnp.float32)
            consume(q)
        for d in range(2):
            view = pf.at[c, turn, :, span2(near[d], d)]
            remote(view, view, s3.at[turn, d, d], r3.at[turn, d, d], pair).wait_recv()
            begin(remote(view, view, s4.at[turn, d], r4.at[turn, d], dev(near[1 - d])))
        for k in range(1, 2 * p):
            there = lax.rem(z + p - lax.rem(k, p), p) * 2 + lax.rem(c + k // p, 2)
            view = qland.at[turn, there]
            remote(view, view, s8.at[turn, k], r8.at[turn, k], pair).wait_recv()
        total = qland[turn, 0]
        for j in range(1, 2 * p):
            total = total + qland[turn, j]
        qsum[turn] = total
        qtot[turn, q] = total
        for k, chip in enumerate(chips):
            begin(remote(qsum.at[turn], qtot.at[turn, q], s9.at[turn, k], r9.at[turn, k], dev(chip)))
        for d in range(2):
            view = pf.at[c, turn, :, span2(near[d], 1 - d)]
            remote(view, view, s3.at[turn, d, 1 - d], r3.at[turn, d, 1 - d], pair).wait_recv()
            view = pf.at[c, turn, :, pl.ds(pl.multiple_of(near[d] * quarter, quarter), quarter)]
            begin(remote(view, view, s5.at[turn, 1 + d], r5.at[turn, 1 + d], pair))
            if turn == 0:
                consume(near[d])
        for d in range(2):
            view = pf.at[c, turn, :, span2(far, d)]
            remote(view, view, s4.at[turn, d], r4.at[turn, d], pair).wait_recv()
            begin(remote(view, view, s5.at[turn, 3 + d], r5.at[turn, 3 + d], pair))
        if turn == 0:
            consume(far)
            for k in range(1, 2 * p):
                begin(remote(msg, mland.at[slot_of], s6.at[k], r6.at[k], group[k - 1]))
            mland[slot_of] = msg[...]

    def curve(turn, direction):
        for k, chip in enumerate(chips):
            view = qtot.at[turn, chip]
            remote(view, view, s9.at[turn, k], r9.at[turn, k], pair).wait_recv()
        total = qtot[turn, 0]
        for j in range(1, 4):
            total = total + qtot[turn, j]
        return small_inverse(total[:, :vecs] + damping * exact_t(direction, direction))

    all_reduce(0)
    direction = dref[...]
    gamma = exact_t(direction, energies)
    alpha = exact(gamma, curve(0, direction))
    gamma_inverse = small_inverse(gamma)
    answer = exact(alpha, direction)
    residual = energies - damping * answer
    for k in range(1, 2 * p):
        there = lax.rem(z + p - lax.rem(k, p), p) * 2 + lax.rem(c + k // p, 2)
        view = mland.at[there]
        remote(view, view, s6.at[k], r6.at[k], pair).wait_recv()
    total = mland[0]
    for j in range(1, 2 * p):
        total = total + mland[j]
    img[:, here] = total
    rres[...] = total
    for k, chip in enumerate(chips):
        begin(remote(rres, img.at[:, here], s7.at[k], r7.at[k], dev(chip)))
    for k, chip in enumerate(chips):
        view = img.at[:, pl.ds(pl.multiple_of(chip * wide, wide), wide)]
        remote(view, view, s7.at[k], r7.at[k], pair).wait_recv()
    residual = residual - exact(alpha, img[...])
    fresh = (residual - exact(exact(exact_t(residual, sketch), inverse), sketch)) / damping
    gamma_next = exact_t(fresh, residual)
    dref[...] = fresh + exact(exact(gamma_next, gamma_inverse), direction)
    all_reduce(1)
    direction = dref[...]
    alpha_next = exact(gamma_next, curve(1, direction))
    dref[...] = answer + exact(alpha_next, direction)
    sol_ref[...] = dref[:, here]
    alpha_ref[0] = alpha
    alpha_ref[1] = alpha_next
    out = pltpu.make_async_copy(pf.at[c], pf_ref.at[c], lsem.at[0, 0])
    out.start()
    for turn in range(2):
        for k, chip in enumerate([q, near[0], near[1]]):
            view = pf.at[o, turn, :, pl.ds(pl.multiple_of(chip * quarter, quarter), quarter)]
            remote(view, view, s5.at[turn, k], r5.at[turn, k], pair).wait_recv()
        for d in range(2):
            view = pf.at[o, turn, :, span2(far, d)]
            remote(view, view, s5.at[turn, 3 + d], r5.at[turn, 3 + d], pair).wait_recv()
    out_two = pltpu.make_async_copy(pf.at[o], pf_ref.at[o], lsem.at[1, 0])
    out_two.start()

    @pl.loop(0, CHUNKS // 2)
    def _(i):
        for d in range(2):
            k = 2 * i + d
            swap(k).wait_send()
            to_pair(k).wait_send()
            for copy in direct(k):
                copy.wait_send()
            forward(k, d).wait_send()

    for copy in auxes + [first] + second + third + [give] + across + spread + sends:
        copy.wait_send()
    out.wait()
    out_two.wait()


def main_call(x, energies, picks, p, total_rows, scale, ident):
    rows, full = x.shape
    half = full // 2
    vecs, count = energies.shape[0], picks.shape[1]
    rank, wide = 8 * count, 2 * rows
    total = 4 * wide
    piece = half // 8
    bf, f32 = jnp.bfloat16, jnp.float32
    vmem, hbm = pl.BlockSpec(memory_space=pltpu.VMEM), pl.BlockSpec(memory_space=pl.ANY)
    smem = pl.BlockSpec(memory_space=pltpu.SMEM)
    dma = lambda *shape: pltpu.SemaphoreType.DMA(shape)
    buf = lambda kind, *shape: pltpu.VMEM(shape, kind)
    return pl.pallas_call(
        functools.partial(main_kernel, p, total_rows, scale),
        out_shape=(
            jax.ShapeDtypeStruct((2, 2, vecs, half), bf),
            jax.ShapeDtypeStruct((2, vecs, vecs), f32),
            jax.ShapeDtypeStruct((vecs, wide), f32),
        ),
        in_specs=[hbm, vmem, smem],
        out_specs=(hbm, vmem, vmem),
        scratch_shapes=[
            buf(bf, rows, half), buf(bf, 2, rows, half), buf(bf, count, half), buf(bf, 8, count, half),
            buf(bf, 2 * count, rows), buf(f32, 2 * count, wide), buf(f32, 8, 2 * count, wide),
            buf(f32, 2, 1, half), buf(f32, 3, 1, half), buf(f32, 1, half), buf(f32, 1, half), buf(f32, 1, half),
            buf(f32, rank, wide), buf(f32, rank // 2, wide), buf(f32, rank // 2, wide),
            buf(f32, p, rank // 2, wide), buf(f32, rank // 2, wide), buf(f32, rank, total),
            buf(f32, rank + vecs, total), buf(f32, rank, 2 * rank), buf(f32, vecs, 128), buf(f32, vecs, total),
            buf(f32, vecs, wide), buf(bf, 2, vecs, half), buf(bf, 2, 2, 2, vecs, piece), buf(bf, 2, 2, vecs, piece),
            buf(f32, 2, vecs, piece), buf(bf, 2, 2, vecs, piece), buf(bf, 2, 2, vecs, half),
            buf(f32, 2, vecs, 128), buf(f32, 2, 2 * p, vecs, 128), buf(f32, 2, vecs, 128),
            buf(f32, 2, 4, vecs, 128), buf(f32, vecs, wide), buf(f32, 2 * p, vecs, wide), buf(f32, vecs, total),
            dma(2, CHUNKS), dma(CHUNKS), dma(CHUNKS), dma(CHUNKS), dma(CHUNKS), dma(2, CHUNKS), dma(2, CHUNKS),
            dma(CHUNKS), dma(CHUNKS), dma(5), dma(5), dma(7), dma(7), dma(p + 7), dma(p + 7),
            dma(2, 2, 2), dma(2, 2, 2), dma(2, 2), dma(2, 2), dma(2, 2, 2), dma(2, 2, 2), dma(2, 2), dma(2, 2),
            dma(2, 5), dma(2, 5), dma(2 * p), dma(2 * p), dma(3), dma(3), dma(2, 2 * p), dma(2, 2 * p),
            dma(2, 3), dma(2, 3),
        ],
        compiler_params=pltpu.CompilerParams(
            collective_id=ident, has_side_effects=True, vmem_limit_bytes=60 * 2**20
        ),
    )(x, energies, picks)


def finish_kernel(pf_ref, alpha_ref, sol_ref, update_ref, out_ref):
    vecs, rows = out_ref.shape
    weights = jnp.concatenate([alpha_ref[0], alpha_ref[1]], axis=1)
    upper = weights.astype(jnp.bfloat16)
    lower = (weights - upper.astype(jnp.float32)).astype(jnp.bfloat16)
    both = jnp.concatenate([upper.astype(jnp.float32), lower.astype(jnp.float32)], axis=0).astype(jnp.bfloat16)
    step = 1024
    for t in range(update_ref.shape[1] // step):
        cols = pl.ds(t * step, step)
        block = pf_ref[0, :, :, cols].astype(jnp.float32).reshape(2 * vecs, step).astype(jnp.bfloat16)
        out = jnp.dot(both, block, preferred_element_type=jnp.float32)
        update_ref[:, cols] = out[:vecs] + out[vecs:]
    core = lax.rem(lax.axis_index("samp"), 2)
    out_ref[...] = jnp.where(core == 0, sol_ref[:, :rows], sol_ref[:, rows:])


def finish_call(pf, alpha, sol):
    _, _, vecs, half = pf.shape
    block = half // 4
    whole = lambda shape: pl.BlockSpec(shape, lambda i: (0,) * len(shape))
    return pl.pallas_call(
        finish_kernel,
        grid=(2 * half // block,),
        out_shape=(
            jax.ShapeDtypeStruct((vecs, 2 * half), jnp.float32),
            jax.ShapeDtypeStruct((vecs, sol.shape[1] // 2), jnp.float32),
        ),
        in_specs=[
            pl.BlockSpec((1, 2, vecs, block), lambda i: (i // 4, 0, 0, i % 4)), whole(alpha.shape), whole(sol.shape)
        ],
        out_specs=(pl.BlockSpec((vecs, block), lambda i: (0, i)), whole((vecs, sol.shape[1] // 2))),
    )(pf, alpha, sol)


def paired_body(log_derivs, energies, nys_rows):
    rows, width = log_derivs.shape
    n, p = lax.axis_size("samp"), lax.axis_size("par")
    pf, alpha, answer = main_call(log_derivs, energies.T, nys_rows, p, n * rows, 1.0 / math.sqrt(width * p), 0)
    update, own = finish_call(pf, alpha, answer)
    return (update.T, own.T)


def solution(mesh):
    n = mesh.shape["samp"]

    def body(log_derivs, energies, nys_rows):
        rows, count = log_derivs.shape[0], energies.shape[1]
        paired = n == 8 and rows == 64 and count == 8 and nys_rows.shape[1] == count
        return (paired_body if paired else general_body)(log_derivs, energies, nys_rows)

    return jax.shard_map(
        body,
        mesh=mesh,
        in_specs=(P("samp", "par"), P("samp", None), P("samp", None)),
        out_specs=(P("par", None), P("samp", None)),
        check_vma=False,
    )
```

```python
import functools
import math

import jax
import jax.numpy as jnp
from jax import lax
from jax.experimental import pallas as pl
from jax.experimental.pallas import tpu as pltpu
from jax.sharding import PartitionSpec as P

ITERS = 2


damping = 0.5

MESH = pl.DeviceIdType.MESH


def factor_solve(factor, right):
    middle = lax.linalg.triangular_solve(factor, right, left_side=True, lower=True)
    return lax.linalg.triangular_solve(factor, middle, left_side=True, lower=True, transpose_a=True)


def eliminate_kernel(matrix_ref, right_ref, out_ref):
    left, right = matrix_ref[...], right_ref[...]
    row = lax.broadcasted_iota(jnp.int32, left.shape, 0)
    for i in range(left.shape[0]):
        column = left[:, i:i + 1]
        pivot = left[i:i + 1, i:i + 1]
        left_row = left[i:i + 1, :] / pivot
        right_row = right[i:i + 1, :] / pivot
        left = jnp.where(row == i, left_row, left - column * left_row)
        right = jnp.where(row == i, right_row, right - column * right_row)
    out_ref[...] = right


def small_solve(matrix, right):
    matrix = 0.5 * (matrix + matrix.T)
    return pl.pallas_call(
        eliminate_kernel, out_shape=jax.ShapeDtypeStruct(right.shape, right.dtype)
    )(matrix, right)


def hdot(left, right):
    return jnp.dot(left, right, precision=lax.Precision.HIGHEST)


def greet(peers):
    barrier = pltpu.get_barrier_semaphore()
    for peer in peers:
        pl.semaphore_signal(barrier, inc=1, device_id=peer, device_id_type=MESH)
    pl.semaphore_wait(barrier, len(peers))


def remote(src, dst, send, recv, peer):
    return pltpu.make_async_remote_copy(
        src_ref=src, dst_ref=dst, send_sem=send, recv_sem=recv, device_id=peer, device_id_type=MESH
    )


def gather_kernel(n, total_rows, scale, sums_ref, aux_ref, chosen_ref, full_ref, sketch_ref, aux_out, centered_out,
                  mean_ref, rows_out, centered_ref, land, own, full, s1, r1, s2, r2, s3, r3, s4, r4, s5, r5, s6, r6, local):
    me, col = lax.axis_index("samp"), lax.axis_index("par")
    at = [lax.rem(me + k, n) for k in range(n)]
    back = [lax.rem(me + n - k, n) for k in range(n)]
    peer = [(at[k], col) for k in range(n)]
    pair = (jnp.bitwise_xor(me, 1), col)
    width = chosen_ref.shape[1]
    half = width // 2
    part = [pl.ds(0, half), pl.ds(half, half)]
    load = pltpu.make_async_copy(full_ref, full, local.at[2])
    load.start()
    greet(peer[1:])
    scatter = [remote(sums_ref.at[at[k]], land.at[k], s1.at[k], r1.at[k], peer[k]) for k in range(1, n)]
    for copy in scatter:
        copy.start()
    sent = list(scatter)
    quad = n == 8
    beside = [jnp.bitwise_xor(me, 2), jnp.bitwise_xor(me, 4)]
    if quad:
        first = [
            remote(chosen_ref.at[:, part[d]], rows_out.at[me, :, part[d]], s4.at[d], r4.at[d], (beside[d], col))
            for d in range(2)
        ]
        for copy in first:
            copy.start()
        sent += first
    auxes = [remote(aux_ref, aux_out.at[me], s2.at[k], r2.at[k], peer[k]) for k in range(1, n)]
    mine = pltpu.make_async_copy(aux_ref, aux_out.at[me], local.at[0])
    mine.start()
    keep = pltpu.make_async_copy(chosen_ref, rows_out.at[me], local.at[1])
    keep.start()
    total = sums_ref[me]
    for k in range(1, n):
        scatter[k - 1].wait_recv()
        total = total + land[k]
    own[...] = total / total_rows
    mean_ref[me] = own[...]
    spread = [remote(own, mean_ref.at[me], s3.at[k], r3.at[k], peer[k]) for k in range(1, n)]
    for copy in spread + auxes:
        copy.start()
    sent += spread + auxes
    over = [remote(chosen_ref, rows_out.at[me], s5.at[0], r5.at[0], pair)]
    over[0].start()
    if quad:
        second = [
            remote(chosen_ref.at[:, part[1 - d]], rows_out.at[me, :, part[1 - d]], s4.at[2 + d], r4.at[2 + d],
                   (beside[d], col))
            for d in range(2)
        ]
        for copy in second:
            copy.start()
        sent += second
        for d in range(2):
            view = rows_out.at[beside[d], :, part[d]]
            remote(view, view, s4.at[d], r4.at[d], pair).wait_recv()
            step = remote(view, view, s4.at[4 + d], r4.at[4 + d], (beside[1 - d], col))
            step.start()
            sent.append(step)
    else:
        far = [remote(chosen_ref, rows_out.at[me], s4.at[k], r4.at[k], peer[k]) for k in range(2, n, 2)]
        for copy in far:
            copy.start()
        sent += far
    for k in range(1, n):
        remote(own, mean_ref.at[back[k]], s3.at[k], r3.at[k], peer[k]).wait_recv()
    load.wait()
    slab = width // n
    tile = math.gcd(slab, 1024)

    @pl.loop(0, n)
    def _(j):
        @pl.loop(0, slab // tile)
        def _(t):
            inner = pl.multiple_of(t * tile, tile)
            cols = pl.ds(pl.multiple_of(j * slab + inner, tile), tile)
            mean = mean_ref[j, :, pl.ds(inner, tile)]
            centered_ref[:, cols] = ((full[:, cols].astype(jnp.float32) - mean) * scale).astype(jnp.bfloat16)

    put = pltpu.make_async_copy(centered_ref, centered_out, local.at[2])
    put.start()
    if quad:
        for d in range(2):
            view = rows_out.at[beside[d], :, part[1 - d]]
            remote(view, view, s4.at[2 + d], r4.at[2 + d], pair).wait_recv()
            block = rows_out.at[beside[d]]
            step = remote(block, block, s5.at[1 + d], r5.at[1 + d], pair)
            step.start()
            over.append(step)
        cross = jnp.bitwise_xor(me, 6)
        for d in range(2):
            view = rows_out.at[cross, :, part[d]]
            remote(view, view, s4.at[4 + d], r4.at[4 + d], pair).wait_recv()
            step = remote(view, view, s5.at[3 + d], r5.at[3 + d], pair)
            step.start()
            over.append(step)
        block = rows_out.at[jnp.bitwise_xor(me, 1)]
        remote(block, block, s5.at[0], r5.at[0], pair).wait_recv()
        for d in range(2):
            block = rows_out.at[jnp.bitwise_xor(me, 3 + 2 * d)]
            remote(block, block, s5.at[1 + d], r5.at[1 + d], pair).wait_recv()
            view = rows_out.at[jnp.bitwise_xor(me, 7), :, part[d]]
            remote(view, view, s5.at[3 + d], r5.at[3 + d], pair).wait_recv()
    else:
        for k in range(2, n, 2):
            block = rows_out.at[back[k]]
            remote(block, block, s4.at[k], r4.at[k], pair).wait_recv()
            step = remote(block, block, s5.at[k], r5.at[k], pair)
            step.start()
            over.append(step)
        for k in range(0, n, 2):
            block = rows_out.at[lax.rem(pair[0] + n - k, n)]
            remote(block, block, s5.at[k], r5.at[k], pair).wait_recv()
    for k in range(1, n):
        remote(aux_ref, aux_out.at[back[k]], s2.at[k], r2.at[k], peer[k]).wait_recv()
    for copy in sent + over:
        copy.wait_send()
    mine.wait()
    keep.wait()
    sketch_ref[...] = jnp.zeros_like(sketch_ref)
    count = n * chosen_ref.shape[0]

    @pl.loop(0, n)
    def _(j):
        @pl.loop(0, slab // tile)
        def _(t):
            inner = pl.multiple_of(t * tile, tile)
            cols = pl.ds(pl.multiple_of(j * slab + inner, tile), tile)
            mean = mean_ref[j, :, pl.ds(inner, tile)]
            rows = rows_out[:, :, cols].astype(jnp.float32).reshape(count, tile)
            rows = ((rows - mean) * scale).astype(jnp.bfloat16)
            sketch_ref[...] += lax.dot_general(
                centered_ref[:, cols], rows, (((1,), (1,)), ((), ())), preferred_element_type=jnp.float32
            )

    put.wait()


def gather_rows(sums, aux, chosen, full, n, total_rows, scale, ident):
    dma = lambda: pltpu.SemaphoreType.DMA((n,))
    vmem = pl.BlockSpec(memory_space=pltpu.VMEM)
    slab = sums.shape[-1]
    return pl.pallas_call(
        functools.partial(gather_kernel, n, total_rows, scale),
        out_shape=(
            jax.ShapeDtypeStruct((full.shape[0], n * chosen.shape[0]), jnp.float32),
            jax.ShapeDtypeStruct((n,) + aux.shape, jnp.float32),
            jax.ShapeDtypeStruct(full.shape, full.dtype),
        ),
        in_specs=[vmem, vmem, vmem, pl.BlockSpec(memory_space=pl.ANY)],
        out_specs=(vmem, vmem, pl.BlockSpec(memory_space=pl.ANY)),
        scratch_shapes=[
            pltpu.VMEM(sums.shape, jnp.float32),
            pltpu.VMEM((n,) + chosen.shape, chosen.dtype),
            pltpu.VMEM(full.shape, full.dtype),
            pltpu.VMEM(sums.shape, jnp.float32),
            pltpu.VMEM((1, slab), jnp.float32),
            pltpu.VMEM(full.shape, full.dtype),
        ] + [dma() for _ in range(12)] + [pltpu.SemaphoreType.DMA((3,))],
        compiler_params=pltpu.CompilerParams(
            collective_id=ident, has_side_effects=True, vmem_limit_bytes=60 * 2**20
        ),
    )(sums, aux, chosen, full)


def spread_kernel(n, p, part_ref, out_ref, land, own, s1, r1, s2, r2):
    me, col = lax.axis_index("samp"), lax.axis_index("par")
    beside = [lax.rem(col + k, p) for k in range(p)]
    at = [lax.rem(me + k, n) for k in range(n)]
    back = [lax.rem(me + n - k, n) for k in range(n)]
    greet([(me, beside[k]) for k in range(1, p)] + [(at[k], col) for k in range(1, n)])
    sums = [remote(part_ref, land.at[col], s1.at[k], r1.at[k], (me, beside[k])) for k in range(1, p)]
    for copy in sums:
        copy.start()
    land[col] = part_ref[...]
    for k in range(1, p):
        there = lax.rem(col + p - k, p)
        remote(part_ref, land.at[there], s1.at[k], r1.at[k], (me, beside[k])).wait_recv()
    total = land[0]
    for j in range(1, p):
        total = total + land[j]
    own[...] = total
    out_ref[me] = total
    hops = [remote(own, out_ref.at[me], s2.at[k], r2.at[k], (at[k], col)) for k in range(1, n)]
    for copy in hops:
        copy.start()
    for k in range(1, n):
        remote(own, out_ref.at[back[k]], s2.at[k], r2.at[k], (at[k], col)).wait_recv()
    for copy in sums + hops:
        copy.wait_send()


def sum_and_spread(part, n, p, ident):
    vmem = pl.BlockSpec(memory_space=pltpu.VMEM)
    return pl.pallas_call(
        functools.partial(spread_kernel, n, p),
        out_shape=jax.ShapeDtypeStruct((n,) + part.shape, jnp.float32),
        in_specs=[vmem],
        out_specs=vmem,
        scratch_shapes=[
            pltpu.VMEM((p,) + part.shape, jnp.float32),
            pltpu.VMEM(part.shape, jnp.float32),
            pltpu.SemaphoreType.DMA((p,)),
            pltpu.SemaphoreType.DMA((p,)),
            pltpu.SemaphoreType.DMA((n,)),
            pltpu.SemaphoreType.DMA((n,)),
        ],
        compiler_params=pltpu.CompilerParams(collective_id=ident, has_side_effects=True),
    )(part)


def reduce_kernel(n, part_ref, out_ref, land, both, inbox, s0, r0, s1, r1, s2, r2, s3, r3):
    me, col = lax.axis_index("samp"), lax.axis_index("par")
    outer = n // 2
    slab = part_ref.shape[1] // n
    half = slab * outer
    i, o = lax.rem(me, 2), me // 2
    pair = (jnp.bitwise_xor(me, 1), col)
    at = [lax.rem(o + k, outer) for k in range(outer)]
    back = [lax.rem(o + outer - k, outer) for k in range(outer)]
    peer = [(at[k] * 2 + i, col) for k in range(outer)]
    cols = lambda j: pl.ds(pl.multiple_of(j * slab, slab), slab)
    halves = lambda j: pl.ds(pl.multiple_of(j * half, half), half)
    greet([pair] + peer[1:])
    swap = remote(part_ref.at[:, halves(1 - i)], land, s0.at[0], r0.at[0], pair)
    swap.start()
    swap.wait_recv()
    both[...] = (part_ref[:, halves(i)].astype(jnp.float32) + land[...].astype(jnp.float32)).astype(both.dtype)
    scatter = [remote(both.at[:, cols(at[k])], inbox.at[k], s1.at[k], r1.at[k], peer[k]) for k in range(1, outer)]
    for copy in scatter:
        copy.start()
    total = part_ref[:, cols(i * outer + o)].astype(jnp.float32) + land[:, cols(o)].astype(jnp.float32)
    for k in range(1, outer):
        scatter[k - 1].wait_recv()
        total = total + inbox[k].astype(jnp.float32)
    home = cols(i * outer + o)
    out_ref[:, home] = total.astype(out_ref.dtype)
    mine = out_ref.at[:, home]
    spread = [remote(mine, mine, s2.at[k], r2.at[k], peer[k]) for k in range(1, outer)]
    spread.append(remote(mine, mine, s3.at[0], r3.at[0], pair))
    for copy in spread:
        copy.start()
    for k in range(1, outer):
        block = out_ref.at[:, cols(i * outer + back[k])]
        remote(block, block, s2.at[k], r2.at[k], pair).wait_recv()
        step = remote(block, block, s3.at[k], r3.at[k], pair)
        step.start()
        spread.append(step)
    for k in range(outer):
        block = out_ref.at[:, cols((1 - i) * outer + back[k])]
        remote(block, block, s3.at[k], r3.at[k], pair).wait_recv()
    for copy in [swap] + scatter + spread:
        copy.wait_send()


def reduce_all(part, n, ident):
    count, width = part.shape
    outer = n // 2
    vmem = pl.BlockSpec(memory_space=pltpu.VMEM)
    return pl.pallas_call(
        functools.partial(reduce_kernel, n),
        out_shape=jax.ShapeDtypeStruct(part.shape, part.dtype),
        in_specs=[vmem],
        out_specs=vmem,
        scratch_shapes=[
            pltpu.VMEM((count, width // 2), part.dtype),
            pltpu.VMEM((count, width // 2), part.dtype),
            pltpu.VMEM((outer, count, width // n), part.dtype),
        ]
        + [pltpu.SemaphoreType.DMA((outer,)) for _ in range(8)],
        compiler_params=pltpu.CompilerParams(collective_id=ident, has_side_effects=True),
    )(part)


def tiny_kernel(p, part_ref, out_ref, land, s1, r1):
    me, col = lax.axis_index("samp"), lax.axis_index("par")
    at = [lax.rem(col + k, p) for k in range(p)]
    back = [lax.rem(col + p - k, p) for k in range(p)]
    greet([(me, at[k]) for k in range(1, p)])
    copies = [remote(part_ref, land.at[col], s1.at[k], r1.at[k], (me, at[k])) for k in range(1, p)]
    for copy in copies:
        copy.start()
    land[col] = part_ref[...]
    for k in range(1, p):
        remote(part_ref, land.at[back[k]], s1.at[k], r1.at[k], (me, at[k])).wait_recv()
    for copy in copies:
        copy.wait_send()
    total = land[0]
    for j in range(1, p):
        total = total + land[j]
    out_ref[...] = total


def tiny_sum(part, p, ident):
    vmem = pl.BlockSpec(memory_space=pltpu.VMEM)
    return pl.pallas_call(
        functools.partial(tiny_kernel, p),
        out_shape=jax.ShapeDtypeStruct(part.shape, part.dtype),
        in_specs=[vmem],
        out_specs=vmem,
        scratch_shapes=[pltpu.VMEM((p,) + part.shape, part.dtype)]
        + [pltpu.SemaphoreType.DMA((p,)) for _ in range(2)],
        compiler_params=pltpu.CompilerParams(collective_id=ident, has_side_effects=True),
    )(part)


def general_body(log_derivs, energies, nys_rows):
    rows, width = log_derivs.shape
    n, p = lax.axis_size("samp"), lax.axis_size("par")
    count, rank = energies.shape[1], nys_rows.shape[1]
    scale = 1.0 / math.sqrt(width * p)
    picks = (nys_rows.reshape(rank, 1) == lax.broadcasted_iota(jnp.int32, (rank, rows), 1)).astype(jnp.bfloat16)
    probe = jnp.concatenate([picks, jnp.ones((8, rows), jnp.bfloat16)], axis=0)
    taken = jnp.dot(probe, log_derivs, preferred_element_type=jnp.float32)
    chosen = taken[:rank].astype(jnp.bfloat16)
    sums = taken[rank].reshape(n, 1, width // n)
    aux = jnp.concatenate([energies, picks.astype(jnp.float32).T], axis=1)
    sketch_part, aux_all, centered = gather_rows(sums, aux, chosen, log_derivs, n, n * rows, scale, 0)
    sketch = sum_and_spread(sketch_part, n, p, 1).reshape(n * rows, n * rank)
    all_energies = aux_all[:, :, :count].reshape(n * rows, count)
    core_block = jnp.einsum(
        "grj,grk->gjk", aux_all[:, :, count:], sketch.reshape(n, rows, n * rank), precision=lax.Precision.HIGHEST
    ).reshape(n * rank, n * rank)
    factor = jnp.linalg.cholesky(damping * core_block + hdot(sketch.T, sketch))

    def precondition(residual):
        coeffs = factor_solve(factor, hdot(sketch.T, residual))
        result = (residual - hdot(sketch, coeffs)) / damping
        return (result, hdot(result.T, residual))

    start = lax.axis_index("samp") * rows
    solution = jnp.zeros(all_energies.shape, jnp.float32)
    update = 0.0
    residual = all_energies
    precond_res, inner_prev = precondition(residual)
    direction = precond_res
    for iteration in range(ITERS):
        rounded = lax.dynamic_slice_in_dim(direction, start, rows, 0).astype(jnp.bfloat16)
        part = jnp.einsum("rv,rc->vc", rounded, centered, preferred_element_type=jnp.float32)
        projected = reduce_all(part.astype(jnp.bfloat16), n, 2 + 2 * iteration)
        if iteration + 1 < ITERS:
            image_part = jnp.einsum("rc,vc->vr", centered, projected, preferred_element_type=jnp.float32)
            image_k = sum_and_spread(image_part, n, p, 3 + 2 * iteration)
            image_k = image_k.transpose(0, 2, 1).reshape(n * rows, count) + damping * direction
            curvature = hdot(direction.T, image_k)
        else:
            square = jnp.einsum("uc,vc->uv", projected, projected, preferred_element_type=jnp.float32)
            curvature = tiny_sum(square, p, 3 + 2 * iteration) + damping * hdot(direction.T, direction)
        alpha_k = small_solve(curvature, inner_prev)
        solution = solution + hdot(direction, alpha_k)
        update = update + hdot(alpha_k.T, projected.astype(jnp.float32))
        if iteration + 1 < ITERS:
            residual = residual - hdot(image_k, alpha_k)
            precond_res, inner_next = precondition(residual)
            beta_k = small_solve(inner_prev, inner_next)
            direction = precond_res + hdot(direction, beta_k)
            inner_prev = inner_next
    return (update.T, lax.dynamic_slice_in_dim(solution, start, rows, 0))


CHUNKS = 8
EARLY = 3
AHEAD = 5
LAG = 2
FINISH = 1


def contract_last(left, right, precision=None):
    return lax.dot_general(
        left, right, (((1,), (1,)), ((), ())), precision=precision, preferred_element_type=jnp.float32
    )


def exact(left, right):
    return jnp.dot(left, right, precision=lax.Precision.HIGHEST, preferred_element_type=jnp.float32)


def exact_t(left, right):
    return contract_last(left, right, lax.Precision.HIGHEST)


def iota(shape, axis):
    return lax.broadcasted_iota(jnp.int32, shape, axis)


def eliminate(matrix, size, group):
    row = iota(matrix.shape, 0)
    lanes = matrix.shape[1]
    for start in range(0, size, group):
        spread = lambda i, j: jnp.broadcast_to(matrix[start + i:start + i + 1, start + j:start + j + 1], (1, lanes))
        cell = [[spread(i, j) for j in range(group)] for i in range(group)]
        for k in range(group):
            inverse = 1.0 / cell[k][k]
            scaled = [cell[k][j] * inverse for j in range(group)]
            for i in range(group):
                if i != k:
                    factor = cell[i][k]
                    cell[i] = [cell[i][j] - factor * scaled[j] for j in range(group)]
                    cell[i][k] = -factor * inverse
            scaled[k] = inverse
            cell[k] = scaled
        old = [matrix[start + j:start + j + 1, :] for j in range(group)]
        fresh = []
        for i in range(group):
            line = cell[i][0] * old[0]
            for j in range(1, group):
                line = line + cell[i][j] * old[j]
            fresh.append(line)
        change = matrix[:, start:start + 1] * fresh[0]
        for i in range(1, group):
            change = change + matrix[:, start + i:start + i + 1] * fresh[i]
        matrix = matrix - change
        for i in range(group):
            matrix = jnp.where(row == start + i, fresh[i], matrix)
    return matrix


def main_kernel(p, total_rows, scale, x_ref, energy_ref, picks_ref, pf, alpha_ref, sol_ref,
                stage, xh, other, rin, probe, aux, aux_all, sums, sland, acc1, acc2, mean, acc, pland, mine, zland,
                tot, sk, aug, big, small, dref, rres, part, land1, mid, keep, land2, sq, qland, qsum, qtot,
                msg, mland, img,
                lsem, wsem, wrecv, psem, precv, osem, rsem, fsem, drecv, bsem, brecv, asem, arecv, tsem, trecv,
                s1, r1, s2, r2, s3, r3, s4, r4, s5, r5, s6, r6, s7, r7, s8, r8, s9, r9):
    me, z = lax.axis_index("samp"), lax.axis_index("par")
    c, q = lax.rem(me, 2), me // 2
    o = 1 - c
    near, far = [jnp.bitwise_xor(q, 1), jnp.bitwise_xor(q, 2)], jnp.bitwise_xor(q, 3)
    rows, half = stage.shape
    wide = 2 * rows
    width = half // CHUNKS
    count = rin.shape[1]
    dev = lambda chip: (chip * 2 + c, z)
    pair = (q * 2 + o, z)
    chips = [near[0], near[1], far]
    span = lambda k: pl.ds(pl.multiple_of(k * width, width), width)
    duo = lambda chip: pl.ds(pl.multiple_of(chip * 2, 2), 2)
    group = [(q * 2 + lax.rem(c + k // p, 2), lax.rem(z + lax.rem(k, p), p)) for k in range(1, 2 * p)]
    samp_peers = [(lax.rem(me + k, 8), z) for k in range(1, 8)]
    par_peers = group[:p - 1]

    def load(k, own):
        core = c if own else o
        cols = pl.ds(pl.multiple_of(core * half + k * width, width), width)
        dst = xh.at[c, :, span(k)] if own else stage.at[:, span(k)]
        return pltpu.make_async_copy(x_ref.at[:, cols], dst, lsem.at[int(own), k])

    barrier = pltpu.get_barrier_semaphore()
    greeted = samp_peers + [peer for k, peer in enumerate(group, 1) if k != p]
    for peer in greeted:
        pl.semaphore_signal(barrier, inc=1, device_id=peer, device_id_type=MESH)

    @pl.loop(0, CHUNKS)
    def _(k):
        load(k, False).start()
        load(k, True).start()

    taken_row, slot = iota((count, rows), 0), iota((count, rows), 1)
    wide_row, wide_slot = iota((count, wide), 0), iota((count, wide), 1)
    picks, wide_picks = jnp.zeros((count, rows), jnp.float32), jnp.zeros((count, wide), jnp.float32)
    for j in range(count):
        at = picks_ref[0, j]
        picks = jnp.where((taken_row == j) & (slot == at), 1.0, picks)
        wide_picks = jnp.where((wide_row == j) & (wide_slot == at + c * rows), 1.0, wide_picks)
    probe[...] = jnp.concatenate([picks, jnp.ones_like(picks)], axis=0).astype(probe.dtype)

    def swap(k):
        return remote(stage.at[:, span(k)], xh.at[c, :, span(k)], wsem.at[k], wrecv.at[k], pair)

    def to_pair(k):
        return remote(other.at[:, span(k)], rin.at[me, :, span(k)], psem.at[k], precv.at[k], pair)

    def direct(k):
        view = rin.at[duo(q), :, span(k)]
        return [remote(view, view, osem.at[d, k], rsem.at[d, k], dev(near[d])) for d in range(2)]

    def forward(k, d):
        view = rin.at[duo(near[d]), :, span(k)]
        return remote(view, view, fsem.at[k], drecv.at[k], dev(near[1 - d]))

    def send(k):
        view = rin.at[me + 1 - 2 * c, :, span(k)]
        remote(view, view, psem.at[k], precv.at[k], pair).wait_recv()
        for copy in direct(k):
            copy.start()

    def relay(k, d):
        for e in range(2):
            view = rin.at[duo(near[e]), :, span(k)]
            remote(view, view, osem.at[e, k], rsem.at[e, k], pair).wait_recv()
        forward(k, d).start()

    def extract(k):
        load(k, False).wait()
        load(k, True).wait()
        step = min(width, 2048)

        @pl.loop(0, width // step)
        def _(s):
            cols = pl.ds(pl.multiple_of(k * width + s * step, step), step)
            theirs = jnp.dot(probe[...], stage[:, cols], preferred_element_type=jnp.float32)
            other[:, cols] = theirs[:count].astype(other.dtype)
            sums[o, :, cols] = theirs[count:count + 1]
            ours = jnp.dot(probe[...], xh[c, :, cols], preferred_element_type=jnp.float32)
            rin[me, :, cols] = ours[:count].astype(rin.dtype)
            sums[c, :, cols] = ours[count:count + 1]

    extract(0)
    pl.semaphore_wait(barrier, len(greeted))
    to_pair(0).start()
    auxes = [remote(aux, aux_all.at[me], asem.at[k], arecv.at[k], samp_peers[k]) for k in range(7)]

    @pl.loop(1, EARLY + 1)
    def _(k):
        extract(k)
        to_pair(k).start()
        send(k - 1)

    @pl.loop(EARLY + 1, CHUNKS)
    def _(k):
        extract(k)
        to_pair(k).start()

    first = remote(sums.at[o], sland.at[0], bsem.at[0], brecv.at[0], pair)
    first.start()

    @pl.loop(0, CHUNKS)
    def _(k):
        swap(k).start()

    place = (iota((rows, wide), 0) + c * rows == iota((rows, wide), 1)).astype(jnp.float32)
    aux[pl.ds(0, count), :] = exact(energy_ref[...], place)
    aux[pl.ds(count, count), :] = wide_picks
    for copy in auxes:
        copy.start()
    aux_all[me] = aux[...]

    first.wait_recv()
    acc1[...] = sums[c] + sland[0]
    part_of = [pl.ds(0, half // 2), pl.ds(half // 2, half // 2)]
    second = [
        remote(acc1.at[:, part_of[d]], sland.at[1, :, part_of[d]], bsem.at[1 + d], brecv.at[1 + d], dev(near[d]))
        for d in range(2)
    ]
    for copy in second:
        copy.start()
    middle = (EARLY + AHEAD) // 2

    @pl.loop(EARLY, middle)
    def _(k):
        send(k)

    for copy in second:
        copy.wait_recv()
    acc2[...] = acc1[...] + sland[1]
    third = [
        remote(acc2.at[:, part_of[d]], sland.at[2, :, part_of[d]], bsem.at[3 + d], brecv.at[3 + d], dev(near[1 - d]))
        for d in range(2)
    ]
    for copy in third:
        copy.start()
    relay(0, 0)

    @pl.loop(middle, AHEAD)
    def _(k):
        send(k)

    relay(1, 1)
    for copy in third:
        copy.wait_recv()
    mean[...] = (acc2[...] + sland[2]) / total_rows
    acc[...] = jnp.zeros_like(acc)

    def process(k):
        remote(stage.at[:, span(k)], xh.at[o, :, span(k)], wsem.at[k], wrecv.at[k], pair).wait_recv()
        view = rin.at[duo(far), :, span(k)]
        remote(view, view, fsem.at[k], drecv.at[k], pair).wait_recv()
        step = min(width, 512)

        @pl.loop(0, width // step)
        def _(s):
            cols = pl.ds(pl.multiple_of(k * width + s * step, step), step)
            shift = mean[:, cols]
            block = xh[:, :, cols].astype(jnp.float32).reshape(wide, step)
            block = ((block - shift) * scale).astype(jnp.bfloat16)
            xh[:, :, cols] = block.reshape(2, rows, step)
            picked = rin[:, :, cols].astype(jnp.float32).reshape(8 * count, step)
            picked = ((picked - shift) * scale).astype(jnp.bfloat16)
            acc[...] += contract_last(picked, block)

    @pl.loop(0, CHUNKS // 2)
    def _(i):
        for d in range(2):
            k = 2 * i + d

            @pl.when(k + AHEAD < CHUNKS)
            def _():
                send(k + AHEAD)

            @pl.when(k + LAG < CHUNKS)
            def _():
                relay(k + LAG, d)

            process(k)

    rank = acc.shape[0]
    own_rows = rank // 2
    mine_rows = pl.ds(pl.multiple_of(c * own_rows, own_rows), own_rows)
    their_rows = pl.ds(pl.multiple_of(o * own_rows, own_rows), own_rows)
    give = remote(acc.at[their_rows], pland, tsem.at[0], trecv.at[0], pair)
    give.start()
    give.wait_recv()
    mine[...] = acc[mine_rows, :] + pland[...]
    across = [remote(mine, zland.at[z], tsem.at[k], trecv.at[k], par_peers[k - 1]) for k in range(1, p)]
    for copy in across:
        copy.start()
    zland[z] = mine[...]
    for k in range(7):
        view = aux_all.at[lax.rem(me + 7 - k, 8)]
        remote(view, view, asem.at[k], arecv.at[k], pair).wait_recv()
    for k in range(1, p):
        view = zland.at[lax.rem(z + p - k, p)]
        remote(view, view, tsem.at[k], trecv.at[k], pair).wait_recv()
    total = zland[0]
    for j in range(1, p):
        total = total + zland[j]
    tot[...] = total
    spot = lambda chip, core: sk.at[
        pl.ds(pl.multiple_of(core * own_rows, own_rows), own_rows),
        pl.ds(pl.multiple_of(chip * wide, wide), wide),
    ]
    here = pl.ds(pl.multiple_of(q * wide, wide), wide)
    sk[mine_rows, here] = total
    spread = [remote(tot, spot(q, c), tsem.at[p + k], trecv.at[p + k], samp_peers[k]) for k in range(7)]
    for copy in spread:
        copy.start()
    @pl.loop(0, CHUNKS // 2)
    def _(i):
        for d in range(2):
            k = 2 * i + d
            swap(k).wait_send()
            to_pair(k).wait_send()
            for copy in direct(k):
                copy.wait_send()
            forward(k, d).wait_send()

    vecs = count
    lower = pl.ds(rank, vecs)
    for chip in range(4):
        cols = pl.ds(chip * wide, wide)
        aug[lower, cols] = aux_all[2 * chip, :vecs, :] + aux_all[2 * chip + 1, :vecs, :]
    energies = aug[lower, :]
    big[...] = (iota(big.shape, 0) + rank == iota(big.shape, 1)).astype(jnp.float32)
    for k in range(7):
        source = lax.rem(me + 7 - k, 8)
        view = spot(source // 2, lax.rem(source, 2))
        remote(view, view, tsem.at[p + k], trecv.at[p + k], pair).wait_recv()

    sketch = sk[...]
    aug[pl.ds(0, rank), :] = sketch
    for g in range(8):
        cols = pl.ds((g // 2) * wide, wide)
        line = pl.ds(g * vecs, vecs)
        aug[line, cols] = aug[line, cols] + damping * aux_all[g, vecs:, :]
    product = exact_t(aug[...], sketch)
    big[:, pl.ds(0, rank)] = product[:rank]
    inverse = eliminate(big[...], rank, 4)[:, rank:2 * rank]
    dref[...] = (energies - exact(exact(product[rank:], inverse), sketch)) / damping

    def small_inverse(matrix):
        small[...] = (iota(small.shape, 0) + vecs == iota(small.shape, 1)).astype(jnp.float32)
        small[:, pl.ds(0, vecs)] = matrix
        return eliminate(small[...], vecs, 4)[:, vecs:2 * vecs]

    quarter = half // 4
    piece = quarter // 2
    span2 = lambda chip, s: pl.ds(pl.multiple_of(chip * quarter + s * piece, piece), piece)
    small_piece = piece // 2
    span3 = lambda chip, s, u: pl.ds(
        pl.multiple_of(chip * quarter + s * piece + u * small_piece, small_piece), small_piece
    )
    step = min(small_piece, 1024)
    slot_of = z * 2 + c
    sends = []

    def begin(copy):
        copy.start()
        sends.append(copy)

    def all_reduce(turn, idle):
        rounded = dref[:, here].astype(jnp.bfloat16)

        def project(chip, s, u):
            for t in range(small_piece // step):
                cols = pl.ds(pl.multiple_of(chip * quarter + s * piece + u * small_piece + t * step, step), step)
                block = xh[:, :, cols].reshape(wide, step)
                part[turn, :, cols] = jnp.dot(rounded, block, preferred_element_type=jnp.float32).astype(part.dtype)

        first_hop, second_hop = {}, {}
        for j in range(2):
            for u in range(2):
                for d in range(2):
                    chip = near[d] if j else far
                    project(chip, d, u)
                    copy = remote(part.at[turn, :, span3(chip, d, u)], land1.at[turn, d, j, u],
                                  s1.at[turn, d, j, u], r1.at[turn, d, j, u], dev(near[d]))
                    first_hop[j, u, d] = copy
                    begin(copy)
        for u in range(2):
            for d in range(2):
                project(near[1 - d], d, u)
        for u in range(2):
            for d in range(2):
                first_hop[0, u, d].wait_recv()
                mid[turn, d, u] = (
                    part[turn, :, span3(near[1 - d], d, u)].astype(jnp.float32)
                    + land1[turn, d, 0, u].astype(jnp.float32)
                ).astype(mid.dtype)
                copy = remote(mid.at[turn, d, u], land2.at[turn, d, u], s2.at[turn, d, u], r2.at[turn, d, u],
                              dev(near[1 - d]))
                second_hop[u, d] = copy
                begin(copy)
        for u in range(2):
            for d in range(2):
                project(q, d, u)
        idle()
        for u in range(2):
            for d in range(2):
                first_hop[1, u, d].wait_recv()
                keep[d, u] = (
                    part[turn, :, span3(q, d, u)].astype(jnp.float32) + land1[turn, d, 1, u].astype(jnp.float32)
                )
        for u in range(2):
            for d in range(2):
                second_hop[u, d].wait_recv()
                pf[c, pl.ds(turn * vecs, vecs), span3(q, d, u)] = (
                    keep[d, u] + land2[turn, d, u].astype(jnp.float32)
                ).astype(pf.dtype)
                view = pf.at[c, pl.ds(turn * vecs, vecs), span3(q, d, u)]
                begin(remote(view, view, s3.at[turn, d, d, u], r3.at[turn, d, d, u], dev(near[d])))
            for d in range(2):
                view = pf.at[c, pl.ds(turn * vecs, vecs), span3(q, 1 - d, u)]
                begin(remote(view, view, s3.at[turn, d, 1 - d, u], r3.at[turn, d, 1 - d, u], dev(near[d])))
        mine_cols = pl.ds(pl.multiple_of(q * quarter, quarter), quarter)
        view = pf.at[c, pl.ds(turn * vecs, vecs), mine_cols]
        begin(remote(view, view, s5.at[turn, 0], r5.at[turn, 0], pair))

        sq[turn] = jnp.zeros(sq.shape[1:], jnp.float32)

        @pl.loop(0, quarter // step)
        def _(t):
            block = pf[c, pl.ds(turn * vecs, vecs), pl.ds(pl.multiple_of(q * quarter + t * step, step), step)]
            sq[turn, :, pl.ds(0, vecs)] += contract_last(block, block)

        for k in range(1, 2 * p):
            begin(remote(sq.at[turn], qland.at[turn, slot_of], s8.at[turn, k], r8.at[turn, k], group[k - 1]))
        qland[turn, slot_of] = sq[turn]

        def consume(chip):
            @pl.loop(0, quarter // step)
            def _(t):
                cols = pl.ds(pl.multiple_of(chip * quarter + t * step, step), step)
                msg[...] += contract_last(pf[c, pl.ds(turn * vecs, vecs), cols], xh[:, :, cols].reshape(wide, step))

        if turn == 0:
            msg[...] = jnp.zeros(msg.shape, jnp.float32)
            consume(q)
        for u in range(2):
            for d in range(2):
                view = pf.at[c, pl.ds(turn * vecs, vecs), span3(near[d], d, u)]
                remote(view, view, s3.at[turn, d, d, u], r3.at[turn, d, d, u], pair).wait_recv()
                begin(remote(view, view, s4.at[turn, d, u], r4.at[turn, d, u], dev(near[1 - d])))
        for k in range(1, 2 * p):
            there = lax.rem(z + p - lax.rem(k, p), p) * 2 + lax.rem(c + k // p, 2)
            view = qland.at[turn, there]
            remote(view, view, s8.at[turn, k], r8.at[turn, k], pair).wait_recv()
        total = qland[turn, 0]
        for j in range(1, 2 * p):
            total = total + qland[turn, j]
        qsum[turn] = total
        qtot[turn, q] = total
        for k, chip in enumerate(chips):
            begin(remote(qsum.at[turn], qtot.at[turn, q], s9.at[turn, k], r9.at[turn, k], dev(chip)))
        for d in range(2):
            for u in range(2):
                view = pf.at[c, pl.ds(turn * vecs, vecs), span3(near[d], 1 - d, u)]
                remote(view, view, s3.at[turn, d, 1 - d, u], r3.at[turn, d, 1 - d, u], pair).wait_recv()
            view = pf.at[c, pl.ds(turn * vecs, vecs), pl.ds(pl.multiple_of(near[d] * quarter, quarter), quarter)]
            begin(remote(view, view, s5.at[turn, 1 + d], r5.at[turn, 1 + d], pair))
            if turn == 0:
                consume(near[d])
        for d in range(2):
            for u in range(2):
                view = pf.at[c, pl.ds(turn * vecs, vecs), span3(far, d, u)]
                remote(view, view, s4.at[turn, d, u], r4.at[turn, d, u], pair).wait_recv()
            view = pf.at[c, pl.ds(turn * vecs, vecs), span2(far, d)]
            begin(remote(view, view, s5.at[turn, 3 + d], r5.at[turn, 3 + d], pair))
        if turn == 0:
            consume(far)
            for k in range(1, 2 * p):
                begin(remote(msg, mland.at[slot_of], s6.at[k], r6.at[k], group[k - 1]))
            mland[slot_of] = msg[...]

    def curve(turn, direction):
        for k, chip in enumerate(chips):
            view = qtot.at[turn, chip]
            remote(view, view, s9.at[turn, k], r9.at[turn, k], pair).wait_recv()
        total = qtot[turn, 0]
        for j in range(1, 4):
            total = total + qtot[turn, j]
        return small_inverse(total[:, :vecs] + damping * exact_t(direction, direction))

    def settle(copies):
        for copy in copies:
            copy.wait_send()

    all_reduce(0, lambda: settle(auxes + [first] + second + third + [give] + across + spread))
    direction = dref[...]
    gamma = exact_t(direction, energies)
    alpha = exact(gamma, curve(0, direction))
    gamma_inverse = small_inverse(gamma)
    answer = exact(alpha, direction)
    residual = energies - damping * answer
    for k in range(1, 2 * p):
        there = lax.rem(z + p - lax.rem(k, p), p) * 2 + lax.rem(c + k // p, 2)
        view = mland.at[there]
        remote(view, view, s6.at[k], r6.at[k], pair).wait_recv()
    total = mland[0]
    for j in range(1, 2 * p):
        total = total + mland[j]
    img[:, here] = total
    rres[...] = total
    for k, chip in enumerate(chips):
        begin(remote(rres, img.at[:, here], s7.at[k], r7.at[k], dev(chip)))
    for k, chip in enumerate(chips):
        view = img.at[:, pl.ds(pl.multiple_of(chip * wide, wide), wide)]
        remote(view, view, s7.at[k], r7.at[k], pair).wait_recv()
    residual = residual - exact(alpha, img[...])
    fresh = (residual - exact(exact(exact_t(residual, sketch), inverse), sketch)) / damping
    gamma_next = exact_t(fresh, residual)
    dref[...] = fresh + exact(exact(gamma_next, gamma_inverse), direction)
    settled = len(sends)
    all_reduce(1, lambda: settle(sends[:settled]))
    direction = dref[...]
    alpha_next = exact(gamma_next, curve(1, direction))
    dref[...] = answer + exact(alpha_next, direction)
    sol_ref[...] = dref[:, here]
    alpha_ref[0] = alpha
    alpha_ref[1] = alpha_next
    for turn in range(2):
        for k, chip in enumerate([q, near[0], near[1]]):
            view = pf.at[o, pl.ds(turn * vecs, vecs), pl.ds(pl.multiple_of(chip * quarter, quarter), quarter)]
            remote(view, view, s5.at[turn, k], r5.at[turn, k], pair).wait_recv()
        for d in range(2):
            view = pf.at[o, pl.ds(turn * vecs, vecs), span2(far, d)]
            remote(view, view, s5.at[turn, 3 + d], r5.at[turn, 3 + d], pair).wait_recv()

    for copy in sends[settled:]:
        copy.wait_send()


def main_call(x, energies, picks, p, total_rows, scale, ident):
    rows, full = x.shape
    half = full // 2
    vecs, count = energies.shape[0], picks.shape[1]
    rank, wide = 8 * count, 2 * rows
    total = 4 * wide
    piece = half // 8
    bf, f32 = jnp.bfloat16, jnp.float32
    vmem, hbm = pl.BlockSpec(memory_space=pltpu.VMEM), pl.BlockSpec(memory_space=pltpu.HBM)
    smem = pl.BlockSpec(memory_space=pltpu.SMEM)
    dma = lambda *shape: pltpu.SemaphoreType.DMA(shape)
    buf = lambda kind, *shape: pltpu.VMEM(shape, kind)
    return pl.pallas_call(
        functools.partial(main_kernel, p, total_rows, scale),
        out_shape=(
            jax.ShapeDtypeStruct((2, 2 * vecs, half), bf),
            jax.ShapeDtypeStruct((2, vecs, vecs), f32),
            jax.ShapeDtypeStruct((vecs, wide), f32),
        ),
        in_specs=[hbm, vmem, smem],
        out_specs=(vmem, vmem, vmem),
        scratch_shapes=[
            buf(bf, rows, half), buf(bf, 2, rows, half), buf(bf, count, half), buf(bf, 8, count, half),
            buf(bf, 2 * count, rows), buf(f32, 2 * count, wide), buf(f32, 8, 2 * count, wide),
            buf(f32, 2, 1, half), buf(f32, 3, 1, half), buf(f32, 1, half), buf(f32, 1, half), buf(f32, 1, half),
            buf(f32, rank, wide), buf(f32, rank // 2, wide), buf(f32, rank // 2, wide),
            buf(f32, p, rank // 2, wide), buf(f32, rank // 2, wide), buf(f32, rank, total),
            buf(f32, rank + vecs, total), buf(f32, rank, 2 * rank), buf(f32, vecs, 128), buf(f32, vecs, total),
            buf(f32, vecs, wide), buf(bf, 2, vecs, half), buf(bf, 2, 2, 2, 2, vecs, piece // 2), buf(bf, 2, 2, 2, vecs, piece // 2),
            buf(f32, 2, 2, vecs, piece // 2), buf(bf, 2, 2, 2, vecs, piece // 2),
            buf(f32, 2, vecs, 128), buf(f32, 2, 2 * p, vecs, 128), buf(f32, 2, vecs, 128),
            buf(f32, 2, 4, vecs, 128), buf(f32, vecs, wide), buf(f32, 2 * p, vecs, wide), buf(f32, vecs, total),
            dma(2, CHUNKS), dma(CHUNKS), dma(CHUNKS), dma(CHUNKS), dma(CHUNKS), dma(2, CHUNKS), dma(2, CHUNKS),
            dma(CHUNKS), dma(CHUNKS), dma(5), dma(5), dma(7), dma(7), dma(p + 7), dma(p + 7),
            dma(2, 2, 2, 2), dma(2, 2, 2, 2), dma(2, 2, 2), dma(2, 2, 2), dma(2, 2, 2, 2), dma(2, 2, 2, 2),
            dma(2, 2, 2), dma(2, 2, 2),
            dma(2, 5), dma(2, 5), dma(2 * p), dma(2 * p), dma(3), dma(3), dma(2, 2 * p), dma(2, 2 * p),
            dma(2, 3), dma(2, 3),
        ],
        compiler_params=pltpu.CompilerParams(
            collective_id=ident, has_side_effects=True, vmem_limit_bytes=48 * 2**20
        ),
    )(x, energies, picks)


def finish_kernel(pf_ref, alpha_ref, sol_ref, update_ref, out_ref):
    vecs, rows = out_ref.shape
    weights = jnp.concatenate([alpha_ref[0], alpha_ref[1]], axis=1)
    upper = weights.astype(jnp.bfloat16)
    lower = (weights - upper.astype(jnp.float32)).astype(jnp.bfloat16)
    both = jnp.concatenate([upper.astype(jnp.float32), lower.astype(jnp.float32)], axis=0).astype(jnp.bfloat16)
    width = update_ref.shape[1]
    per_core = pf_ref.shape[2] // width
    i = pl.program_id(0)
    step = min(width, 1024)
    for t in range(width // step):
        cols = pl.ds(pl.multiple_of(lax.rem(i, per_core) * width + t * step, step), step)
        out = jnp.dot(both, pf_ref[i // per_core, :, cols], preferred_element_type=jnp.float32)
        update_ref[:, pl.ds(t * step, step)] = out[:vecs] + out[vecs:]
    core = lax.rem(lax.axis_index("samp"), 2)
    out_ref[...] = jnp.where(core == 0, sol_ref[:, :rows], sol_ref[:, rows:])


def finish_call(pf, alpha, sol):
    _, vecs, half = pf.shape
    vecs = vecs // 2
    block = half // FINISH
    vmem = pl.BlockSpec(memory_space=pltpu.VMEM)
    own = (vecs, sol.shape[1] // 2)
    return pl.pallas_call(
        finish_kernel,
        grid=(2 * half // block,),
        out_shape=(jax.ShapeDtypeStruct((vecs, 2 * half), jnp.float32), jax.ShapeDtypeStruct(own, jnp.float32)),
        in_specs=[vmem, vmem, vmem],
        out_specs=(pl.BlockSpec((vecs, block), lambda i: (0, i)), pl.BlockSpec(own, lambda i: (0, 0))),
        compiler_params=pltpu.CompilerParams(vmem_limit_bytes=8 * 2**20),
    )(pf, alpha, sol)


def paired_body(log_derivs, energies, nys_rows):
    rows, width = log_derivs.shape
    n, p = lax.axis_size("samp"), lax.axis_size("par")
    pf, alpha, answer = main_call(log_derivs, energies.T, nys_rows, p, n * rows, 1.0 / math.sqrt(width * p), 0)
    update, own = finish_call(pf, alpha, answer)
    return (update.T, own.T)


def solution(mesh):
    n = mesh.shape["samp"]

    def body(log_derivs, energies, nys_rows):
        rows, count = log_derivs.shape[0], energies.shape[1]
        paired = n == 8 and rows == 64 and count == 8 and nys_rows.shape[1] == count
        return (paired_body if paired else general_body)(log_derivs, energies, nys_rows)

    return jax.shard_map(
        body,
        mesh=mesh,
        in_specs=(P("samp", "par"), P("samp", None), P("samp", None)),
        out_specs=(P("par", None), P("samp", None)),
        check_vma=False,
    )
```
